32 devices in a mesh: wa: 4 (over z), bl: 8 (over y, x, core).
Axes of the slice: x: 2, y: 2, z: 4, core: 2. Of those that a mesh axis runs over, the one named last changes fastest.
Arguments:
- visibilities: float32 [4, 16, 2, 128], P('wa', 'bl'), may hold values from -6 to 6
- weights: float32 [4, 16, 128], P('wa', 'bl'), may hold values from 0.25 to 4
- cell_index: int32 [4, 16, 128], P('wa', 'bl'), may hold values from 0 to 1048575
- kernel_index: int32 [4, 16, 128], P('wa', 'bl'), may hold values from 0 to 255
- layer_index: int32 [4, 16, 128], P('wa', 'bl'), may hold values from 0 to 1
- tile_counts: int32 [4, 16], P('wa', 'bl'), may hold values from 1 to 128
- kernel_table: float32 [16, 8], replicated, may hold values from 0.05 to 0.3
- layer_depth: float32 [8], P('wa'), may hold values from -150 to 150
Outputs:
- image: float32 [1024, 1024], P('wa', 'bl')
The draws below stay inside these ranges and needn't reach their ends.
All inputs are finite; a program needn't handle non-finite values.
Results may differ from the reference program's by a relative error of at most 0.0003.
Values sent between devices are 32-bit elements; how exact they have to be, the bound alone decides.
No kernel may reach another device: no remote copies, remote signals or barrier semaphores. Data moves between devices by JAX's collectives and lax.ppermute only.
A program may use at most 128 MiB of HBM per device.

```python
import math
import jax
import jax.numpy as jnp
from jax import lax

GRID = 1024
SUPPORT = 8
OVERSAMPLE = 16
SAMPLES = 128
LAYER_DEV = 2
WGROUPS = 4
LAYERS = 8
TILES = 16


def place_ends(drawn, key, least, top_value):
    extent = drawn.shape
    place = [jax.random.randint(jax.random.fold_in(key, axis), (), 0, extent[axis]) for axis in range(len(extent))]
    drawn = drawn.at[tuple(place)].set(least)
    longest = extent.index(max(extent))
    place[longest] = (place[longest] + 1) % extent[longest]
    return drawn.at[tuple(place)].set(top_value)


def block_scale(own_key, dims, pieces, low, largest):
    def one(dim, parts):
        draws = jax.random.uniform(jax.random.fold_in(jax.random.fold_in(own_key, 6), dim), (parts,), jnp.float32, low / len(pieces), largest / len(pieces))
        return jnp.repeat(jnp.exp(draws), dims[dim] // parts).reshape((-1,) + (1,) * (len(dims) - dim - 1))

    gain = one(*pieces[0])
    for cut in pieces[1:]:
        gain = gain * one(*cut)
    return gain


def scatter_about(key, shape, spread, bound, split=(), kind=jnp.bfloat16):
    loudness = block_scale(key, shape, split, -0.22, 0.18) if split else 1.0
    array = jax.random.normal(key, shape, jnp.float32) * spread * loudness
    return jnp.minimum(jnp.maximum(array, -bound), bound).astype(kind)


def setup_inputs(seed: int = 0) -> dict:
    seeds = jax.random.split(jax.random.key(seed), 9)
    visibilities = scatter_about(seeds[0], (WGROUPS, TILES, 2, SAMPLES), 1.0, 6.0, ((0, 4), (1, 8)), jnp.float32)
    weights = jnp.clip(jnp.exp(math.log(4.0) - 2.7725887 * jax.random.uniform(seeds[1], (WGROUPS, TILES, SAMPLES), jnp.float32) ** block_scale(seeds[1], (WGROUPS, TILES, SAMPLES), ((0, 4), (1, 8)), -0.2, 0.2)), 0.25, 4.0)
    cell_index = place_ends(jax.random.randint(seeds[2], (WGROUPS, TILES, SAMPLES), 0, GRID * GRID), jax.random.fold_in(seeds[2], 1), 0, (GRID * GRID) - 1).astype(jnp.int32)
    kernel_index = place_ends(jax.random.randint(seeds[3], (WGROUPS, TILES, SAMPLES), 0, OVERSAMPLE * OVERSAMPLE), jax.random.fold_in(seeds[3], 1), 0, (OVERSAMPLE * OVERSAMPLE) - 1).astype(jnp.int32)
    layer_index = place_ends(jax.random.randint(seeds[4], (WGROUPS, TILES, SAMPLES), 0, LAYER_DEV), jax.random.fold_in(seeds[4], 1), 0, LAYER_DEV - 1).astype(jnp.int32)
    tile_counts = place_ends(jax.random.randint(seeds[5], (WGROUPS, TILES), 1, SAMPLES + 1), jax.random.fold_in(seeds[5], 1), 1, SAMPLES).astype(jnp.int32)
    kernel_table = jnp.clip(jax.random.uniform(seeds[6], (OVERSAMPLE, SUPPORT), jnp.float32, 0.05, 0.3), 0.05, 0.3)
    layer_depth = jnp.clip(jax.random.uniform(seeds[7], (LAYERS,), jnp.float32, -150.0, 150.0) * block_scale(seeds[7], (LAYERS,), ((0, 4),), -0.4, 0.0), -150.0, 150.0)
    return dict(visibilities=visibilities, weights=weights, cell_index=cell_index, kernel_index=kernel_index, layer_index=layer_index, tile_counts=tile_counts, kernel_table=kernel_table, layer_depth=layer_depth)


field_of_view = 0.6

def reference(visibilities, weights, cell_index, kernel_index, layer_index, tile_counts, kernel_table, layer_depth):
    position = lax.broadcasted_iota(jnp.int32, cell_index.shape, 2)
    usable = position < tile_counts[:, :, None]
    used_weight = jnp.where(usable, weights, jnp.float32(0.0))
    square_sum = jnp.sum(used_weight * used_weight)
    group_index = lax.broadcasted_iota(jnp.int32, cell_index.shape, 0)
    global_layer = group_index * LAYER_DEV + layer_index
    row_cell = cell_index // GRID
    col_cell = cell_index % GRID
    row_kernel = kernel_table[kernel_index // OVERSAMPLE]
    col_kernel = kernel_table[kernel_index % OVERSAMPLE]
    offsets = jnp.arange(SUPPORT, dtype=jnp.int32) - SUPPORT // 2
    row_target = (row_cell[..., None] + offsets) % GRID
    col_target = (col_cell[..., None] + offsets) % GRID
    amount = row_kernel[..., :, None] * col_kernel[..., None, :]
    vis_real = visibilities[:, :, 0, :] * used_weight
    vis_imag = visibilities[:, :, 1, :] * used_weight
    layer_cells = global_layer[..., None, None]
    row_cells = row_target[..., :, None]
    col_cells = col_target[..., None, :]
    grid_real = jnp.zeros((LAYERS, GRID, GRID), jnp.float32).at[layer_cells, row_cells, col_cells].add(vis_real[..., None, None] * amount)
    grid_imag = jnp.zeros((LAYERS, GRID, GRID), jnp.float32).at[layer_cells, row_cells, col_cells].add(vis_imag[..., None, None] * amount)
    coords = (jnp.arange(GRID, dtype=jnp.int32) - GRID // 2).astype(jnp.float32) * (field_of_view / GRID)
    depth_term = jnp.sqrt(1.0 - coords[:, None] * coords[:, None] - coords[None, :] * coords[None, :]) - 1.0

    def add_layer(accumulated, layer_item):
        part_real, part_imag, depth_value = layer_item
        spectrum = jnp.fft.ifft2(part_real + 1j * part_imag) * (GRID * GRID)
        phases = 2.0 * jnp.pi * depth_value * depth_term
        return (accumulated + (jnp.real(spectrum) * jnp.cos(phases) - jnp.imag(spectrum) * jnp.sin(phases)), None)
    screened, unused = lax.scan(add_layer, jnp.zeros((GRID, GRID), jnp.float32), (grid_real, grid_imag, layer_depth))
    return screened / jnp.sqrt(square_sum)
```

```python
import functools
import math

import jax
import jax.numpy as jnp
from jax import lax
from jax.experimental import pallas as pl
from jax.experimental.pallas import tpu as pltpu
from jax.sharding import PartitionSpec as P

GRID = 1024
SUPPORT = 8
OVERSAMPLE = 16
FIELD_OF_VIEW = 0.6

LANES = 128
LOW = LANES // OVERSAMPLE
FIELDS = 4

highest = lax.Precision.HIGHEST
last_dims = (((1,), (1,)), ((), ()))

COS_TERMS = (2.4433157e-5, -1.3887316e-3, 4.1666646e-2, -0.5, 1.0)
SIN_TERMS = (-1.9515296e-4, 8.3321609e-3, -1.6666655e-1, 1.0)


def iota(shape, dim):
    return lax.broadcasted_iota(jnp.int32, shape, dim)


def quarter_wave(angle, quarter):
    square = angle * angle
    cosine = jnp.full_like(square, COS_TERMS[0])
    for term in COS_TERMS[1:]:
        cosine = cosine * square + term
    sine = jnp.full_like(square, SIN_TERMS[0])
    for term in SIN_TERMS[1:]:
        sine = sine * square + term
    sine = sine * angle
    odd = (quarter & 1) == 1
    first = jnp.where(odd, sine, cosine)
    second = jnp.where(odd, cosine, sine)
    first = jnp.where(((quarter + 1) & 2) == 2, -first, first)
    second = jnp.where((quarter & 2) == 2, -second, second)
    return first, second


def unit_root(power):
    moved = (power & (GRID - 1)) + GRID // 8
    step = (moved & (GRID // 4 - 1)) - GRID // 8
    return quarter_wave(step.astype(jnp.float32) * (2.0 * math.pi / GRID), moved // (GRID // 4))


def split_two(value):
    upper = value.astype(jnp.bfloat16)
    return upper, (value - upper.astype(jnp.float32)).astype(jnp.bfloat16)


def pack_kernel(layer_dev, count_ref, depth_ref, vis_ref, weight_ref, cell_ref, kernel_ref, layer_ref, out_ref):
    tiles, samples = weight_ref.shape
    slots = tiles * samples
    lane = iota((1, samples), 1)
    rows = []
    used_weight = []
    for tile in range(tiles):
        used = lane < count_ref[0, tile]
        used_weight.append(jnp.where(used, weight_ref[tile : tile + 1, :], 0.0))
        for layer in range(layer_dev):
            rows.append(jnp.where(used & (layer_ref[tile : tile + 1, :] == layer), 1.0, 0.0))
    mask = jnp.concatenate(rows, axis=0)
    upper = jnp.where(iota((samples, samples), 0) <= iota((samples, samples), 1), 1.0, 0.0)
    rank = jnp.dot(
        mask.astype(jnp.bfloat16), upper.astype(jnp.bfloat16), preferred_element_type=jnp.float32
    )
    total = jnp.sum(mask, axis=1, keepdims=True)
    base = jnp.zeros((1, 1), jnp.float32)
    layer_count = []
    target = [jnp.full((1, samples), -1.0, jnp.float32) for tile in range(tiles)]
    for layer in range(layer_dev):
        start = base
        for tile in range(tiles):
            row = tile * layer_dev + layer
            place = base + rank[row : row + 1, :] - 1.0
            target[tile] = jnp.where(mask[row : row + 1, :] > 0.0, place, target[tile])
            base = base + total[row : row + 1, :]
        layer_count.append(base - start)
    target = jnp.concatenate(target, axis=1).astype(jnp.int32)
    chosen = jnp.where(iota((slots, slots), 0) == target, 1.0, 0.0).astype(jnp.bfloat16)
    weight_row = jnp.concatenate(used_weight, axis=1)
    real_row = jnp.concatenate([vis_ref[2 * t : 2 * t + 1, :] for t in range(tiles)], axis=1)
    imag_row = jnp.concatenate([vis_ref[2 * t + 1 : 2 * t + 2, :] for t in range(tiles)], axis=1)
    cell_row = jnp.concatenate([cell_ref[t : t + 1, :] for t in range(tiles)], axis=1)
    kernel_row = jnp.concatenate([kernel_ref[t : t + 1, :] for t in range(tiles)], axis=1)
    fields = jnp.concatenate(
        [
            real_row * weight_row,
            imag_row * weight_row,
            cell_row.astype(jnp.float32),
            kernel_row.astype(jnp.float32),
        ],
        axis=0,
    )
    parts = []
    for part in range(3):
        upper_part = fields.astype(jnp.bfloat16)
        parts.append(upper_part.astype(jnp.float32))
        fields = fields - upper_part.astype(jnp.float32)
    moved = lax.dot_general(
        jnp.concatenate(parts, axis=0).astype(jnp.bfloat16),
        chosen,
        last_dims,
        preferred_element_type=jnp.float32,
    )
    out_ref[:, :slots] = moved[:FIELDS] + moved[FIELDS : 2 * FIELDS] + moved[2 * FIELDS :]
    wide = iota((FIELDS, LANES), 1)
    extra = jnp.zeros((FIELDS, LANES), jnp.float32)
    square = jnp.sum(weight_row * weight_row, axis=1, keepdims=True)
    extra = jnp.where(wide == 2 * layer_dev, square, extra)
    for layer in range(layer_dev):
        extra = jnp.where(wide == layer, layer_count[layer], extra)
        extra = jnp.where(wide == layer_dev + layer, depth_ref[layer], extra)
    out_ref[:, slots:] = extra


def image_kernel(
    layer_dev,
    groups,
    members,
    slot_ref,
    table_ref,
    out_ref,
    extra_ref,
    stream_ref,
    first_u,
    second_u,
    first_v,
    second_v,
    left_zero,
    left_one,
    right_zero,
    right_one,
    sum_ref,
    place_ref,
    owner_ref,
    valid_ref,
    copy_sem,
):
    rows, columns = out_ref.shape
    wide = first_v.shape[1]
    slots = slot_ref.shape[2] - LANES
    source_tiles = slots // LANES
    regions = groups * layer_dev
    region_tiles = stream_ref.shape[0] // regions
    row_start = lax.axis_index("wa") * rows
    column_start = lax.axis_index("bl") * columns

    copy = pltpu.make_async_copy(slot_ref.at[:, pl.ds(0, 1), pl.ds(slots, LANES)], extra_ref, copy_sem)
    copy.start()

    low_lane = iota((OVERSAMPLE, LANES), 1) % LOW
    position_lane = iota((OVERSAMPLE, LANES), 1) // LOW
    picked = jnp.where(position_lane == iota((OVERSAMPLE, LANES), 0), 1.0, 0.0)
    taps = lax.dot_general(
        table_ref[...], picked, (((0,), (0,)), ((), ())), precision=highest, preferred_element_type=jnp.float32
    )
    band = jnp.zeros((OVERSAMPLE, LANES), jnp.float32)
    for tap in range(SUPPORT):
        band = jnp.where(iota((OVERSAMPLE, LANES), 0) - low_lane == tap, taps[tap : tap + 1, :], band)

    def fill(first, second, start):
        count = first.shape[1]
        pixel = start + iota((count, OVERSAMPLE), 0)
        roots = unit_root((iota((count, OVERSAMPLE), 1) - SUPPORT // 2) * pixel)
        for part in range(2):
            first[part] = jnp.dot(roots[part], band, precision=highest, preferred_element_type=jnp.float32)
        count = second.shape[1]
        pixel = start + iota((count, LANES), 0)
        roots = unit_root(iota((count, LANES), 1) * LOW * pixel)
        for part in range(2):
            second[part] = roots[part]

    fill(first_u, second_u, row_start)
    fill(first_v, second_v, column_start)
    sum_ref[...] = jnp.zeros_like(sum_ref)
    copy.wait()

    lane = iota((FIELDS, LANES), 1)

    def join(group, filled_tiles):
        base = [0] * layer_dev
        for member in range(members):
            device = group * members + member
            source = [slot_ref[device, :, LANES * t : LANES * (t + 1)] for t in range(source_tiles)]
            origin = 0
            for layer in range(layer_dev):
                count = extra_ref[device, 0, layer].astype(jnp.int32)
                offset = base[layer] - origin
                shift = offset & (LANES - 1)
                tile = offset >> 7
                turned = [pltpu.roll(part, shift, 1) for part in source]
                region = (group * layer_dev + layer) * region_tiles + source_tiles
                for t in range(source_tiles + 1):
                    if t == 0:
                        value = turned[0]
                    elif t == source_tiles:
                        value = turned[t - 1]
                    else:
                        value = jnp.where(lane >= shift, turned[t], turned[t - 1])
                    where = region + tile + t
                    keep = lane < base[layer] - (tile + t) * LANES
                    stream_ref[where] = jnp.where(keep, stream_ref[where], value)
                base[layer] = base[layer] + count
                origin = origin + count
        for layer in range(layer_dev):
            number = (base[layer] + LANES - 1) >> 7

            def enter(tile, unused):
                place_ref[filled_tiles + tile] = (group * layer_dev + layer) * region_tiles + source_tiles + tile
                owner_ref[filled_tiles + tile] = group * layer_dev + layer
                valid_ref[filled_tiles + tile] = base[layer] - tile * LANES
                return unused

            lax.fori_loop(0, number, enter, 0)
            filled_tiles = filled_tiles + number
        return filled_tiles

    tile_total = lax.fori_loop(0, groups, join, 0)
    for spare in range(3):
        place_ref[tile_total + spare] = source_tiles
        owner_ref[tile_total + spare] = 0
        valid_ref[tile_total + spare] = 0

    def build(tile, left, right):
        content = stream_ref[place_ref[tile]]
        live = iota((1, LANES), 1) < valid_ref[tile]
        real = jnp.where(live, content[0:1], 0.0)
        imag = jnp.where(live, content[1:2], 0.0)
        cell = jnp.where(live, content[2:3], 0.0).astype(jnp.int32)
        kernel = jnp.where(live, content[3:4], 0.0).astype(jnp.int32)
        row = cell // GRID
        column = cell % GRID

        def spread(line):
            return jnp.broadcast_to(line, (8, LANES))

        row_first = spread((kernel // OVERSAMPLE) * LOW + row % LOW)
        row_second = spread(row // LOW)
        column_first = spread((kernel % OVERSAMPLE) * LOW + column % LOW)
        column_second = spread(column // LOW)

        def pick(ref, part, at, index):
            return jnp.take_along_axis(ref[part, at : at + 8, :], index, axis=1, mode="promise_in_bounds")

        period = second_u.shape[1]
        for at in range(0, period, 16):
            second = [
                [pick(second_u, part, at + half, row_second) for half in (0, 8)] for part in range(2)
            ]
            second = [jnp.concatenate(halves, axis=0) for halves in second]
            for again in range(at, rows, period):
                first = [
                    jnp.concatenate([pick(first_u, part, again + half, row_first) for half in (0, 8)], axis=0)
                    for part in range(2)
                ]
                parts = (
                    first[0] * second[0] - first[1] * second[1],
                    first[0] * second[1] + first[1] * second[0],
                )
                for part in range(2):
                    upper, lower = split_two(parts[part])
                    left[0, again : again + 16, LANES * part : LANES * (part + 1)] = upper
                    left[1, again : again + 16, LANES * part : LANES * (part + 1)] = lower
        real = jnp.broadcast_to(real, (16, LANES))
        imag = jnp.broadcast_to(imag, (16, LANES))
        for at in range(0, wide, 16):
            first = [
                jnp.concatenate([pick(first_v, part, at + half, column_first) for half in (0, 8)], axis=0)
                for part in range(2)
            ]
            second = [
                jnp.concatenate([pick(second_v, part, at + half, column_second) for half in (0, 8)], axis=0)
                for part in range(2)
            ]
            both = (
                first[0] * second[0] - first[1] * second[1],
                first[0] * second[1] + first[1] * second[0],
            )
            weighted = (both[0] * real - both[1] * imag, both[0] * imag + both[1] * real)
            for level, (value_real, value_imag) in enumerate(zip(split_two(weighted[0]), split_two(weighted[1]))):
                right[level, at : at + 16, :LANES] = value_real
                right[level, at : at + 16, LANES:] = -value_imag
                right[level, wide + at : wide + at + 16, :LANES] = value_imag
                right[level, wide + at : wide + at + 16, LANES:] = value_real

    def add(tile, left, right):
        owner = owner_ref[tile]
        product = lax.dot_general(
            jnp.concatenate([left[0], left[1], left[0]], axis=1),
            jnp.concatenate([right[0], right[0], right[1]], axis=1),
            last_dims,
            preferred_element_type=jnp.float32,
        )
        sum_ref[owner] = sum_ref[owner] + product

    build(0, left_zero, right_zero)

    def pair(step, unused):
        add(2 * step, left_zero, right_zero)
        build(2 * step + 1, left_one, right_one)
        add(2 * step + 1, left_one, right_one)
        build(2 * step + 2, left_zero, right_zero)
        return unused

    lax.fori_loop(0, (tile_total + 1) // 2, pair, 0)

    square_sum = lax.fori_loop(
        0, groups * members, lambda d, total: total + extra_ref[d, 0, 2 * layer_dev], jnp.float32(0.0)
    )
    scale = 1.0 / jnp.sqrt(jnp.full((1, wide), square_sum, jnp.float32))
    pixel_size = FIELD_OF_VIEW / GRID
    chunk = 16

    def screen(step, unused):
        at = pl.multiple_of(step * chunk, chunk)
        x_coord = (row_start + at + iota((chunk, wide), 0) - GRID // 2).astype(jnp.float32) * pixel_size
        y_coord = (column_start + iota((chunk, wide), 1) - GRID // 2).astype(jnp.float32) * pixel_size
        inside = 1.0 - x_coord * x_coord - y_coord * y_coord
        depth = jnp.sqrt(inside) - 1.0
        total = jnp.zeros((chunk, wide), jnp.float32)
        for region in range(regions):
            layer_depth = extra_ref[region // layer_dev * members, 0, layer_dev + region % layer_dev]
            quarters = (4.0 * layer_depth) * depth
            nearest = jnp.round(quarters)
            angle = (quarters - nearest) * (0.5 * math.pi)
            cosine, sine = quarter_wave(angle, nearest.astype(jnp.int32))
            total = total + sum_ref[region, pl.ds(at, chunk), :wide] * cosine
            total = total - sum_ref[region, pl.ds(at, chunk), wide:] * sine
        out_ref[pl.ds(at, chunk), :] = (total * scale)[:, :columns]
        return unused

    lax.fori_loop(0, rows // chunk, screen, 0)


def body(
    visibilities,
    weights,
    cell_index,
    kernel_index,
    layer_index,
    tile_counts,
    kernel_table,
    layer_depth,
):
    layer_dev = layer_depth.shape[0]
    groups, members = lax.axis_size("wa"), lax.axis_size("bl")
    tiles, samples = cell_index.shape[1:]
    slots = tiles * samples
    rows, columns = GRID // groups, GRID // members
    wide = max(columns, LANES)
    vmem = pl.BlockSpec(memory_space=pltpu.VMEM)
    smem = pl.BlockSpec(memory_space=pltpu.SMEM)
    packed = pl.pallas_call(
        functools.partial(pack_kernel, layer_dev),
        out_shape=jax.ShapeDtypeStruct((FIELDS, slots + LANES), jnp.float32),
        in_specs=[smem, smem, vmem, vmem, vmem, vmem, vmem],
        out_specs=vmem,
        name="pack_slots",
    )(
        tile_counts,
        layer_depth,
        visibilities.reshape(2 * tiles, samples),
        weights.reshape(tiles, samples),
        cell_index.reshape(tiles, samples),
        kernel_index.reshape(tiles, samples),
        layer_index.reshape(tiles, samples),
    )
    devices = groups * members
    copies = jnp.broadcast_to(packed[None], (devices,) + packed.shape)
    gathered = lax.all_to_all(copies, ("wa", "bl"), split_axis=0, concat_axis=0, tiled=True)
    region_tiles = members * slots // LANES + 2 * (slots // LANES) + 1
    most_tiles = devices * slots // LANES + groups * layer_dev + 4
    period = min(rows, LANES)
    return pl.pallas_call(
        functools.partial(image_kernel, layer_dev, groups, members),
        out_shape=jax.ShapeDtypeStruct((rows, columns), jnp.float32),
        in_specs=[vmem, vmem],
        out_specs=vmem,
        scratch_shapes=[
            pltpu.SMEM((devices, 1, LANES), jnp.float32),
            pltpu.VMEM((groups * layer_dev * region_tiles, FIELDS, LANES), jnp.float32),
            pltpu.VMEM((2, rows, LANES), jnp.float32),
            pltpu.VMEM((2, period, LANES), jnp.float32),
            pltpu.VMEM((2, wide, LANES), jnp.float32),
            pltpu.VMEM((2, wide, LANES), jnp.float32),
            pltpu.VMEM((2, rows, 2 * LANES), jnp.bfloat16),
            pltpu.VMEM((2, rows, 2 * LANES), jnp.bfloat16),
            pltpu.VMEM((2, 2 * wide, 2 * LANES), jnp.bfloat16),
            pltpu.VMEM((2, 2 * wide, 2 * LANES), jnp.bfloat16),
            pltpu.VMEM((groups * layer_dev, rows, 2 * wide), jnp.float32),
            pltpu.SMEM((most_tiles,), jnp.int32),
            pltpu.SMEM((most_tiles,), jnp.int32),
            pltpu.SMEM((most_tiles,), jnp.int32),
            pltpu.SemaphoreType.DMA,
        ],
        name="slots_to_image",
    )(gathered, kernel_table)


def solution(mesh):
    in_specs = (
        P("wa", "bl", None, None),
        P("wa", "bl", None),
        P("wa", "bl", None),
        P("wa", "bl", None),
        P("wa", "bl", None),
        P("wa", "bl"),
        P(),
        P("wa"),
    )
    return jax.shard_map(body, mesh=mesh, in_specs=in_specs, out_specs=P("wa", "bl"), check_vma=False)
```

```python
import functools
import math

import jax
import jax.numpy as jnp
from jax import lax
from jax.experimental import pallas as pl
from jax.experimental.pallas import tpu as pltpu
from jax.sharding import PartitionSpec as P

GRID = 1024
SUPPORT = 8
OVERSAMPLE = 16
FIELD_OF_VIEW = 0.6

LANES = 128
LOW = LANES // OVERSAMPLE
FIELDS = 4

highest = lax.Precision.HIGHEST
last_dims = (((1,), (1,)), ((), ()))

COS_TERMS = (0.2196967899799347, -1.3318802118301392, 4.058412075042725, -4.934792995452881, 0.9999999403953552)
SIN_TERMS = (0.0772201269865036, -0.5980451703071594, 2.5500314235687256, -5.1677069664001465, 3.141592502593994)
GRID_BITS = GRID.bit_length() - 1
LOW_BITS = LOW.bit_length() - 1
POSITION_BITS = OVERSAMPLE.bit_length() - 1


def iota(shape, dim):
    return lax.broadcasted_iota(jnp.int32, shape, dim)


def half_turn(value):
    square = value * value
    cosine = jnp.full_like(square, COS_TERMS[0])
    for term in COS_TERMS[1:]:
        cosine = cosine * square + term
    sine = jnp.full_like(square, SIN_TERMS[0])
    for term in SIN_TERMS[1:]:
        sine = sine * square + term
    return cosine, sine * value


def unit_root(power):
    moved = power + GRID // 4
    step = (moved & (GRID // 2 - 1)) - GRID // 4
    cosine, sine = half_turn(step.astype(jnp.float32) * (2.0 / GRID))
    flip = (moved & (GRID // 2)) != 0
    return jnp.where(flip, -cosine, cosine), jnp.where(flip, -sine, sine)


def split_two(value):
    upper = value.astype(jnp.bfloat16)
    return upper, (value - upper.astype(jnp.float32)).astype(jnp.bfloat16)


def pack_kernel(layer_dev, count_ref, depth_ref, vis_ref, weight_ref, cell_ref, kernel_ref, layer_ref, out_ref):
    tiles, samples = weight_ref.shape
    slots = tiles * samples
    lane = iota((1, samples), 1)
    rows = []
    used_weight = []
    for tile in range(tiles):
        used = lane < count_ref[0, tile]
        used_weight.append(jnp.where(used, weight_ref[tile : tile + 1, :], 0.0))
        for layer in range(layer_dev):
            rows.append(jnp.where(used & (layer_ref[tile : tile + 1, :] == layer), 1.0, 0.0))
    mask = jnp.concatenate(rows, axis=0)
    upper = jnp.where(iota((samples, samples), 0) <= iota((samples, samples), 1), 1.0, 0.0)
    rank = jnp.dot(
        mask.astype(jnp.bfloat16), upper.astype(jnp.bfloat16), preferred_element_type=jnp.float32
    )
    total = jnp.sum(mask, axis=1, keepdims=True)
    base = jnp.zeros((1, 1), jnp.float32)
    layer_count = []
    target = [jnp.full((1, samples), -1.0, jnp.float32) for tile in range(tiles)]
    for layer in range(layer_dev):
        start = base
        for tile in range(tiles):
            row = tile * layer_dev + layer
            place = base + rank[row : row + 1, :] - 1.0
            target[tile] = jnp.where(mask[row : row + 1, :] > 0.0, place, target[tile])
            base = base + total[row : row + 1, :]
        layer_count.append(base - start)
    target = jnp.concatenate(target, axis=1).astype(jnp.int32)
    chosen = jnp.where(iota((slots, slots), 0) == target, 1.0, 0.0).astype(jnp.bfloat16)
    weight_row = jnp.concatenate(used_weight, axis=1)
    real_row = jnp.concatenate([vis_ref[2 * t : 2 * t + 1, :] for t in range(tiles)], axis=1)
    imag_row = jnp.concatenate([vis_ref[2 * t + 1 : 2 * t + 2, :] for t in range(tiles)], axis=1)
    cell_row = jnp.concatenate([cell_ref[t : t + 1, :] for t in range(tiles)], axis=1)
    kernel_row = jnp.concatenate([kernel_ref[t : t + 1, :] for t in range(tiles)], axis=1)
    fields = jnp.concatenate(
        [
            real_row * weight_row,
            imag_row * weight_row,
            cell_row.astype(jnp.float32),
            kernel_row.astype(jnp.float32),
        ],
        axis=0,
    )
    parts = []
    for part in range(3):
        upper_part = fields.astype(jnp.bfloat16)
        parts.append(upper_part.astype(jnp.float32))
        fields = fields - upper_part.astype(jnp.float32)
    moved = lax.dot_general(
        jnp.concatenate(parts, axis=0).astype(jnp.bfloat16),
        chosen,
        last_dims,
        preferred_element_type=jnp.float32,
    )
    moved = moved[:FIELDS] + moved[FIELDS : 2 * FIELDS] + moved[2 * FIELDS :]
    wide = iota((FIELDS, LANES), 1)
    extra = jnp.zeros((FIELDS, LANES), jnp.float32)
    square = jnp.sum(weight_row * weight_row, axis=1, keepdims=True)
    extra = jnp.where(wide == 2 * layer_dev, square, extra)
    for layer in range(layer_dev):
        extra = jnp.where(wide == layer, layer_count[layer], extra)
        extra = jnp.where(wide == layer_dev + layer, depth_ref[layer], extra)
    for device in range(out_ref.shape[0]):
        out_ref[device, :, :slots] = moved
        out_ref[device, :, slots:] = extra


def table_kernel(taps_ref, first_u, second_u, first_v, second_v, depth_ref):
    rows, columns = depth_ref.shape
    row_start = lax.axis_index("wa") * rows
    column_start = lax.axis_index("bl") * (GRID // lax.axis_size("bl"))
    low_lane = iota((OVERSAMPLE, LANES), 1) & (LOW - 1)
    position_lane = iota((OVERSAMPLE, LANES), 1) >> LOW_BITS
    picked = jnp.where(position_lane == iota((OVERSAMPLE, LANES), 0), 1.0, 0.0)
    taps = jnp.dot(taps_ref[...], picked, precision=highest, preferred_element_type=jnp.float32)
    band = jnp.zeros((OVERSAMPLE, LANES), jnp.float32)
    for tap in range(SUPPORT):
        band = jnp.where(iota((OVERSAMPLE, LANES), 0) - low_lane == tap, taps[tap : tap + 1, :], band)

    def fill(first, second, start):
        count = first.shape[1]
        pixel = start + iota((count, OVERSAMPLE), 0)
        roots = unit_root((iota((count, OVERSAMPLE), 1) - SUPPORT // 2) * pixel)
        for part in range(2):
            first[part] = jnp.dot(roots[part], band, precision=highest, preferred_element_type=jnp.float32)
        count = second.shape[1]
        pixel = start + iota((count, LANES), 0)
        roots = unit_root(iota((count, LANES), 1) * LOW * pixel)
        for part in range(2):
            second[part] = roots[part]

    fill(first_u, second_u, row_start)
    fill(first_v, second_v, column_start)
    pixel_size = FIELD_OF_VIEW / GRID
    x_coord = (row_start + iota((rows, columns), 0) - GRID // 2).astype(jnp.float32) * pixel_size
    y_coord = (column_start + iota((rows, columns), 1) - GRID // 2).astype(jnp.float32) * pixel_size
    depth_ref[...] = jnp.sqrt(jnp.maximum(1.0 - x_coord * x_coord - y_coord * y_coord, 0.0)) - 1.0


def image_kernel(
    layer_dev,
    groups,
    members,
    slot_ref,
    first_u,
    second_u,
    first_v,
    second_v,
    depth_ref,
    out_ref,
    extra_ref,
    stream_ref,
    index_refs,
    value_refs,
    left_refs,
    right_refs,
    sum_ref,
    place_ref,
    owner_ref,
    valid_ref,
    copy_sem,
):
    rows, columns = out_ref.shape
    wide = first_v.shape[1]
    slots = slot_ref.shape[2] - LANES
    source_tiles = slots // LANES
    regions = groups * layer_dev
    region_tiles = stream_ref.shape[0] // regions

    copy = pltpu.make_async_copy(slot_ref.at[:, pl.ds(0, 1), pl.ds(slots, LANES)], extra_ref, copy_sem)
    copy.start()
    sum_ref[...] = jnp.zeros_like(sum_ref)
    copy.wait()

    lane = iota((FIELDS, LANES), 1)

    def join(group, filled_tiles):
        base = [0] * layer_dev
        for member in range(members):
            device = group * members + member
            source = [slot_ref[device, :, LANES * t : LANES * (t + 1)] for t in range(source_tiles)]
            origin = 0
            for layer in range(layer_dev):
                count = extra_ref[device, 0, layer].astype(jnp.int32)
                offset = base[layer] - origin
                shift = offset & (LANES - 1)
                tile = offset >> 7
                turned = [pltpu.roll(part, shift, 1) for part in source]
                region = (group * layer_dev + layer) * region_tiles + source_tiles
                for t in range(source_tiles + 1):
                    if t == 0:
                        value = turned[0]
                    elif t == source_tiles:
                        value = turned[t - 1]
                    else:
                        value = jnp.where(lane >= shift, turned[t], turned[t - 1])
                    where = region + tile + t
                    keep = lane < base[layer] - (tile + t) * LANES
                    stream_ref[where] = jnp.where(keep, stream_ref[where], value)
                base[layer] = base[layer] + count
                origin = origin + count
        for layer in range(layer_dev):
            number = (base[layer] + LANES - 1) >> 7

            def enter(tile, unused):
                place_ref[filled_tiles + tile] = (group * layer_dev + layer) * region_tiles + source_tiles + tile
                owner_ref[filled_tiles + tile] = group * layer_dev + layer
                valid_ref[filled_tiles + tile] = base[layer] - tile * LANES
                return unused

            lax.fori_loop(0, number, enter, 0)
            filled_tiles = filled_tiles + number
        return filled_tiles

    tile_total = lax.fori_loop(0, groups, join, 0)
    for spare in range(8):
        place_ref[tile_total + spare] = source_tiles
        owner_ref[tile_total + spare] = 0
        valid_ref[tile_total + spare] = 0

    def prepare(tile, parity, side):
        content = stream_ref[place_ref[tile]]
        live = iota((1, LANES), 1) < valid_ref[tile]
        cell = jnp.where(live, content[2:3], 0.0).astype(jnp.int32)
        kernel = jnp.where(live, content[3:4], 0.0).astype(jnp.int32)
        row = cell >> GRID_BITS
        column = cell & (GRID - 1)
        value, index = value_refs[parity][side], index_refs[parity][side]
        value[0:1] = jnp.where(live, content[0:1], 0.0)
        value[1:2] = jnp.where(live, content[1:2], 0.0)
        index[0:1] = ((kernel >> POSITION_BITS) << LOW_BITS) + (row & (LOW - 1))
        index[1:2] = row >> LOW_BITS
        index[2:3] = ((kernel & (OVERSAMPLE - 1)) << LOW_BITS) + (column & (LOW - 1))
        index[3:4] = column >> LOW_BITS

    def build(parity, side):
        left, right = left_refs[parity][side], right_refs[parity][side]
        index = [jnp.broadcast_to(index_refs[parity][side][k : k + 1], (8, LANES)) for k in range(4)]
        real = jnp.broadcast_to(value_refs[parity][side][0:1], (16, LANES))
        imag = jnp.broadcast_to(value_refs[parity][side][1:2], (16, LANES))

        def pick(ref, at, which):
            return [
                jnp.concatenate(
                    [
                        jnp.take_along_axis(
                            ref[part, at + half : at + half + 8], index[which], axis=1, mode="promise_in_bounds"
                        )
                        for half in (0, 8)
                    ],
                    axis=0,
                )
                for part in range(2)
            ]

        def times(one, two):
            return one[0] * two[0] - one[1] * two[1], one[0] * two[1] + one[1] * two[0]

        period = second_u.shape[1]
        for at in range(0, period, 16):
            second = pick(second_u, at, 1)
            for again in range(at, rows, period):
                both = times(pick(first_u, again, 0), second)
                for part in range(2):
                    upper, lower = split_two(both[part])
                    left[0, part, again : again + 16] = upper
                    left[1, part, again : again + 16] = lower
        for at in range(0, wide, 16):
            both = times(times(pick(first_v, at, 2), pick(second_v, at, 3)), (real, imag))
            for level, (value_real, value_imag) in enumerate(zip(split_two(both[0]), split_two(both[1]))):
                right[level, 0, at : at + 16] = value_real
                right[level, 1, at : at + 16] = -value_imag
                right[level, 0, wide + at : wide + at + 16] = value_imag
                right[level, 1, wide + at : wide + at + 16] = value_real

    def add(tile, parity, side):
        left, right = left_refs[parity][side], right_refs[parity][side]
        owner = owner_ref[tile]
        product = lax.dot_general(
            jnp.concatenate([left[level, part] for level in (0, 1, 0) for part in range(2)], axis=1),
            jnp.concatenate([right[level, part] for level in (0, 0, 1) for part in range(2)], axis=1),
            last_dims,
            preferred_element_type=jnp.float32,
        )
        sum_ref[owner] = sum_ref[owner] + product

    for side in range(2):
        prepare(side, 0, side)
        prepare(2 + side, 1, side)
    for side in range(2):
        build(0, side)

    def four(step, unused):
        for parity in range(2):
            tile = 4 * step + 2 * parity
            for side in range(2):
                add(tile + side, parity, side)
            for side in range(2):
                build(1 - parity, side)
            for side in range(2):
                prepare(tile + 4 + side, parity, side)
        return unused

    lax.fori_loop(0, (tile_total + 3) // 4, four, 0)

    square_sum = jnp.float32(0.0)
    for device in range(groups * members):
        square_sum = square_sum + extra_ref[device, 0, 2 * layer_dev]
    scale = 1.0 / jnp.sqrt(jnp.full((1, wide), square_sum, jnp.float32))
    chunk = 16

    def screen(step, unused):
        at = pl.multiple_of(step * chunk, chunk)
        depth = depth_ref[pl.ds(at, chunk), :]
        total = jnp.zeros((chunk, wide), jnp.float32)
        for region in range(regions):
            layer_depth = extra_ref[region // layer_dev * members, 0, layer_dev + region % layer_dev]
            halves = (2.0 * layer_depth) * depth
            nearest = jnp.round(halves)
            cosine, sine = half_turn(halves - nearest)
            part = sum_ref[region, pl.ds(at, chunk), :wide] * cosine
            part = part - sum_ref[region, pl.ds(at, chunk), wide:] * sine
            total = total + jnp.where((nearest.astype(jnp.int32) & 1) == 1, -part, part)
        out_ref[pl.ds(at, chunk), :] = (total * scale)[:, :columns]
        return unused

    lax.fori_loop(0, rows // chunk, screen, 0)


def body(
    visibilities,
    weights,
    cell_index,
    kernel_index,
    layer_index,
    tile_counts,
    kernel_table,
    layer_depth,
):
    layer_dev = layer_depth.shape[0]
    groups, members = lax.axis_size("wa"), lax.axis_size("bl")
    tiles, samples = cell_index.shape[1:]
    slots = tiles * samples
    rows, columns = GRID // groups, GRID // members
    wide = max(columns, LANES)
    vmem = pl.BlockSpec(memory_space=pltpu.VMEM)
    smem = pl.BlockSpec(memory_space=pltpu.SMEM)
    devices = groups * members
    packed = pl.pallas_call(
        functools.partial(pack_kernel, layer_dev),
        out_shape=jax.ShapeDtypeStruct((devices, FIELDS, slots + LANES), jnp.float32),
        in_specs=[smem, smem, vmem, vmem, vmem, vmem, vmem],
        out_specs=vmem,
        compiler_params=pltpu.CompilerParams(vmem_limit_bytes=4 << 20),
        name="pack_slots",
    )(
        tile_counts,
        layer_depth,
        visibilities.reshape(2 * tiles, samples),
        weights.reshape(tiles, samples),
        cell_index.reshape(tiles, samples),
        kernel_index.reshape(tiles, samples),
        layer_index.reshape(tiles, samples),
    )
    gathered = lax.all_to_all(packed, ("wa", "bl"), split_axis=0, concat_axis=0, tiled=True)
    period = min(rows, LANES)
    shapes = [(2, rows, LANES), (2, period, LANES), (2, wide, LANES), (2, wide, LANES), (rows, wide)]
    tables = pl.pallas_call(
        table_kernel,
        out_shape=[jax.ShapeDtypeStruct(shape, jnp.float32) for shape in shapes],
        in_specs=[vmem],
        out_specs=[vmem] * len(shapes),
        compiler_params=pltpu.CompilerParams(vmem_limit_bytes=8 << 20),
        cost_estimate=pl.CostEstimate(flops=8000000, bytes_accessed=1000000, transcendentals=0),
        name="lane_tables",
    )(kernel_table.T)
    region_tiles = members * slots // LANES + 2 * (slots // LANES) + 1
    most_tiles = devices * slots // LANES + groups * layer_dev + 8

    def four_of(shape, kind):
        return [[pltpu.VMEM(shape, kind) for side in range(2)] for parity in range(2)]

    return pl.pallas_call(
        functools.partial(image_kernel, layer_dev, groups, members),
        out_shape=jax.ShapeDtypeStruct((rows, columns), jnp.float32),
        in_specs=[vmem] * (1 + len(shapes)),
        out_specs=vmem,
        scratch_shapes=[
            pltpu.SMEM((devices, 1, LANES), jnp.float32),
            pltpu.VMEM((groups * layer_dev * region_tiles, FIELDS, LANES), jnp.float32),
            four_of((8, LANES), jnp.int32),
            four_of((8, LANES), jnp.float32),
            four_of((2, 2, rows, LANES), jnp.bfloat16),
            four_of((2, 2, 2 * wide, LANES), jnp.bfloat16),
            pltpu.VMEM((groups * layer_dev, rows, 2 * wide), jnp.float32),
            pltpu.SMEM((most_tiles,), jnp.int32),
            pltpu.SMEM((most_tiles,), jnp.int32),
            pltpu.SMEM((most_tiles,), jnp.int32),
            pltpu.SemaphoreType.DMA,
        ],
        compiler_params=pltpu.CompilerParams(vmem_limit_bytes=24 << 20),
        name="slots_to_image",
    )(gathered, *tables)


def solution(mesh):
    in_specs = (
        P("wa", "bl", None, None),
        P("wa", "bl", None),
        P("wa", "bl", None),
        P("wa", "bl", None),
        P("wa", "bl", None),
        P("wa", "bl"),
        P(),
        P("wa"),
    )
    return jax.shard_map(body, mesh=mesh, in_specs=in_specs, out_specs=P("wa", "bl"), check_vma=False)
```

```python
import functools
import math

import jax
import jax.numpy as jnp
from jax import lax
from jax.experimental import pallas as pl
from jax.experimental.pallas import tpu as pltpu
from jax.sharding import PartitionSpec as P

GRID = 1024
SUPPORT = 8
OVERSAMPLE = 16
FIELD_OF_VIEW = 0.6

LANES = 128
LOW = LANES // OVERSAMPLE
FIELDS = 4

highest = lax.Precision.HIGHEST
last_dims = (((1,), (1,)), ((), ()))

COS_TERMS = (0.2196967899799347, -1.3318802118301392, 4.058412075042725, -4.934792995452881, 0.9999999403953552)
SIN_TERMS = (0.0772201269865036, -0.5980451703071594, 2.5500314235687256, -5.1677069664001465, 3.141592502593994)
GRID_BITS = GRID.bit_length() - 1
LOW_BITS = LOW.bit_length() - 1
POSITION_BITS = OVERSAMPLE.bit_length() - 1


def iota(shape, dim):
    return lax.broadcasted_iota(jnp.int32, shape, dim)


def half_turn(value):
    square = value * value
    cosine = jnp.full_like(square, COS_TERMS[0])
    for term in COS_TERMS[1:]:
        cosine = cosine * square + term
    sine = jnp.full_like(square, SIN_TERMS[0])
    for term in SIN_TERMS[1:]:
        sine = sine * square + term
    return cosine, sine * value


def unit_root(power):
    moved = power + GRID // 4
    step = (moved & (GRID // 2 - 1)) - GRID // 4
    cosine, sine = half_turn(step.astype(jnp.float32) * (2.0 / GRID))
    flip = (moved & (GRID // 2)) != 0
    return jnp.where(flip, -cosine, cosine), jnp.where(flip, -sine, sine)


def split_two(value):
    upper = value.astype(jnp.bfloat16)
    return upper, (value - upper.astype(jnp.float32)).astype(jnp.bfloat16)


def pack_kernel(layer_dev, count_ref, depth_ref, vis_ref, weight_ref, cell_ref, kernel_ref, layer_ref, out_ref):
    tiles, samples = weight_ref.shape
    slots = tiles * samples
    lane = iota((1, samples), 1)
    rows = []
    used_weight = []
    for tile in range(tiles):
        used = lane < count_ref[0, tile]
        used_weight.append(jnp.where(used, weight_ref[tile : tile + 1, :], 0.0))
        for layer in range(layer_dev):
            rows.append(jnp.where(used & (layer_ref[tile : tile + 1, :] == layer), 1.0, 0.0))
    mask = jnp.concatenate(rows, axis=0)
    upper = jnp.where(iota((samples, samples), 0) <= iota((samples, samples), 1), 1.0, 0.0)
    rank = jnp.dot(
        mask.astype(jnp.bfloat16), upper.astype(jnp.bfloat16), preferred_element_type=jnp.float32
    )
    total = jnp.sum(mask, axis=1, keepdims=True)
    base = jnp.zeros((1, 1), jnp.float32)
    layer_count = []
    target = [jnp.full((1, samples), -1.0, jnp.float32) for tile in range(tiles)]
    for layer in range(layer_dev):
        start = base
        for tile in range(tiles):
            row = tile * layer_dev + layer
            place = base + rank[row : row + 1, :] - 1.0
            target[tile] = jnp.where(mask[row : row + 1, :] > 0.0, place, target[tile])
            base = base + total[row : row + 1, :]
        layer_count.append(base - start)
    target = jnp.concatenate(target, axis=1).astype(jnp.int32)
    chosen = jnp.where(iota((slots, slots), 0) == target, 1.0, 0.0).astype(jnp.bfloat16)
    weight_row = jnp.concatenate(used_weight, axis=1)
    real_row = jnp.concatenate([vis_ref[2 * t : 2 * t + 1, :] for t in range(tiles)], axis=1)
    imag_row = jnp.concatenate([vis_ref[2 * t + 1 : 2 * t + 2, :] for t in range(tiles)], axis=1)
    cell_row = jnp.concatenate([cell_ref[t : t + 1, :] for t in range(tiles)], axis=1)
    kernel_row = jnp.concatenate([kernel_ref[t : t + 1, :] for t in range(tiles)], axis=1)
    fields = jnp.concatenate(
        [
            real_row * weight_row,
            imag_row * weight_row,
            cell_row.astype(jnp.float32),
            kernel_row.astype(jnp.float32),
        ],
        axis=0,
    )
    parts = []
    for part in range(3):
        upper_part = fields.astype(jnp.bfloat16)
        parts.append(upper_part.astype(jnp.float32))
        fields = fields - upper_part.astype(jnp.float32)
    moved = lax.dot_general(
        jnp.concatenate(parts, axis=0).astype(jnp.bfloat16),
        chosen,
        last_dims,
        preferred_element_type=jnp.float32,
    )
    moved = moved[:FIELDS] + moved[FIELDS : 2 * FIELDS] + moved[2 * FIELDS :]
    wide = iota((FIELDS, LANES), 1)
    extra = jnp.zeros((FIELDS, LANES), jnp.float32)
    square = jnp.sum(weight_row * weight_row, axis=1, keepdims=True)
    extra = jnp.where(wide == 2 * layer_dev, square, extra)
    for layer in range(layer_dev):
        extra = jnp.where(wide == layer, layer_count[layer], extra)
        extra = jnp.where(wide == layer_dev + layer, depth_ref[layer], extra)
    for device in range(out_ref.shape[0]):
        out_ref[device, :, :slots] = moved
        out_ref[device, :, slots:] = extra


def table_kernel(taps_ref, first_u, base_u, step_u, first_v, base_v, step_v, depth_ref):
    rows, columns = depth_ref.shape
    row_start = lax.axis_index("wa") * rows
    column_start = lax.axis_index("bl") * (GRID // lax.axis_size("bl"))
    low_lane = iota((OVERSAMPLE, LANES), 1) & (LOW - 1)
    position_lane = iota((OVERSAMPLE, LANES), 1) >> LOW_BITS
    picked = jnp.where(position_lane == iota((OVERSAMPLE, LANES), 0), 1.0, 0.0)
    taps = jnp.dot(taps_ref[...], picked, precision=highest, preferred_element_type=jnp.float32)
    band = jnp.zeros((OVERSAMPLE, LANES), jnp.float32)
    for tap in range(SUPPORT):
        band = jnp.where(iota((OVERSAMPLE, LANES), 0) - low_lane == tap, taps[tap : tap + 1, :], band)

    def fill(first, base, step, start):
        count = first.shape[1]
        pixel = start + iota((count, OVERSAMPLE), 0)
        roots = unit_root((iota((count, OVERSAMPLE), 1) - SUPPORT // 2) * pixel)
        for part in range(2):
            first[part] = jnp.dot(roots[part], band, precision=highest, preferred_element_type=jnp.float32)
        roots = unit_root(iota((8, LANES), 1) * LOW * (start + iota((8, LANES), 0)))
        for part in range(2):
            base[part] = roots[part]
        count = step.shape[1]
        roots = unit_root(iota((count, LANES), 1) * LOW * 8 * iota((count, LANES), 0))
        for part in range(2):
            step[part] = roots[part]

    fill(first_u, base_u, step_u, row_start)
    fill(first_v, base_v, step_v, column_start)
    pixel_size = FIELD_OF_VIEW / GRID
    x_coord = (row_start + iota((rows, columns), 0) - GRID // 2).astype(jnp.float32) * pixel_size
    y_coord = (column_start + iota((rows, columns), 1) - GRID // 2).astype(jnp.float32) * pixel_size
    depth_ref[...] = jnp.sqrt(jnp.maximum(1.0 - x_coord * x_coord - y_coord * y_coord, 0.0)) - 1.0


def image_kernel(
    layer_dev,
    groups,
    members,
    slot_ref,
    first_u,
    base_u,
    step_u,
    first_v,
    base_v,
    step_v,
    depth_ref,
    out_ref,
    extra_ref,
    stream_ref,
    index_refs,
    wave_refs,
    left_refs,
    right_refs,
    sum_ref,
    place_ref,
    owner_ref,
    valid_ref,
    copy_sem,
):
    rows, columns = out_ref.shape
    wide = first_v.shape[1]
    slots = slot_ref.shape[2] - LANES
    source_tiles = slots // LANES
    regions = groups * layer_dev
    region_tiles = stream_ref.shape[0] // regions

    copy = pltpu.make_async_copy(slot_ref.at[:, pl.ds(0, 1), pl.ds(slots, LANES)], extra_ref, copy_sem)
    copy.start()
    sum_ref[...] = jnp.zeros_like(sum_ref)
    copy.wait()

    lane = iota((FIELDS, LANES), 1)

    def join(group, filled_tiles):
        base = [0] * layer_dev
        for member in range(members):
            device = group * members + member
            source = [slot_ref[device, :, LANES * t : LANES * (t + 1)] for t in range(source_tiles)]
            origin = 0
            for layer in range(layer_dev):
                count = extra_ref[device, 0, layer].astype(jnp.int32)
                offset = base[layer] - origin
                shift = offset & (LANES - 1)
                tile = offset >> 7
                turned = [pltpu.roll(part, shift, 1) for part in source]
                region = (group * layer_dev + layer) * region_tiles + source_tiles
                for t in range(source_tiles + 1):
                    if t == 0:
                        value = turned[0]
                    elif t == source_tiles:
                        value = turned[t - 1]
                    else:
                        value = jnp.where(lane >= shift, turned[t], turned[t - 1])
                    where = region + tile + t
                    keep = lane < base[layer] - (tile + t) * LANES
                    stream_ref[where] = jnp.where(keep, stream_ref[where], value)
                base[layer] = base[layer] + count
                origin = origin + count
        for layer in range(layer_dev):
            number = (base[layer] + LANES - 1) >> 7

            def enter(tile, unused):
                place_ref[filled_tiles + tile] = (group * layer_dev + layer) * region_tiles + source_tiles + tile
                owner_ref[filled_tiles + tile] = group * layer_dev + layer
                valid_ref[filled_tiles + tile] = base[layer] - tile * LANES
                return unused

            lax.fori_loop(0, number, enter, 0)
            filled_tiles = filled_tiles + number
        return filled_tiles

    tile_total = lax.fori_loop(0, groups, join, 0)
    for spare in range(8):
        place_ref[tile_total + spare] = source_tiles
        owner_ref[tile_total + spare] = 0
        valid_ref[tile_total + spare] = 0

    steps_u, steps_v = step_u.shape[1], step_v.shape[1]

    def pick(ref, at, index):
        return [
            jnp.take_along_axis(ref[part, at : at + 8], index, axis=1, mode="promise_in_bounds") for part in range(2)
        ]

    def times(one, two):
        return one[0] * two[0] - one[1] * two[1], one[0] * two[1] + one[1] * two[0]

    def prepare(tile, parity, side):
        content = stream_ref[place_ref[tile]]
        live = iota((1, LANES), 1) < valid_ref[tile]
        cell = jnp.where(live, content[2:3], 0.0).astype(jnp.int32)
        kernel = jnp.where(live, content[3:4], 0.0).astype(jnp.int32)
        row = cell >> GRID_BITS
        column = cell & (GRID - 1)
        index, wave = index_refs[parity][side], wave_refs[parity][side]
        index[0:1] = ((kernel >> POSITION_BITS) << LOW_BITS) + (row & (LOW - 1))
        index[1:2] = ((kernel & (OVERSAMPLE - 1)) << LOW_BITS) + (column & (LOW - 1))
        row_high = jnp.broadcast_to(row >> LOW_BITS, (8, LANES))
        column_high = jnp.broadcast_to(column >> LOW_BITS, (8, LANES))
        value = [jnp.broadcast_to(jnp.where(live, content[part : part + 1], 0.0), (8, LANES)) for part in range(2)]
        bases = (pick(base_u, 0, row_high), times(pick(base_v, 0, column_high), value))
        at = 0
        for base, step, high in zip(bases, (step_u, step_v), (row_high, column_high)):
            for part in range(2):
                wave[part, at : at + 8] = base[part]
            at = at + 8
            for block in range(0, step.shape[1], 8):
                picked = pick(step, block, high)
                for part in range(2):
                    wave[part, at : at + 8] = picked[part]
                at = at + 8

    def build(parity, side):
        left, right = left_refs[parity][side], right_refs[parity][side]
        wave = wave_refs[parity][side]
        row_index, column_index = [
            jnp.broadcast_to(index_refs[parity][side][k : k + 1], (8, LANES)) for k in range(2)
        ]
        row_base = [wave[part, 0:8] for part in range(2)]
        column_base = [wave[part, 8 + steps_u : 16 + steps_u] for part in range(2)]

        def turn(base, at):
            return times(base, [jnp.broadcast_to(wave[part, at : at + 1], (8, LANES)) for part in range(2)])

        def paired(low, high):
            return [split_two(jnp.concatenate([low[part], high[part]], axis=0)) for part in range(2)]

        period = 8 * steps_u
        for at in range(0, period, 16):
            second = [turn(row_base, 8 + (at + half) // 8) for half in (0, 8)]
            for again in range(at, rows, period):
                both = paired(*[times(pick(first_u, again + 8 * k, row_index), second[k]) for k in range(2)])
                for part in range(2):
                    for level in range(2):
                        left[level, part, again : again + 16] = both[part][level]
        for at in range(0, wide, 16):
            second = [turn(column_base, 16 + steps_u + (at + half) // 8) for half in (0, 8)]
            both = paired(*[times(pick(first_v, at + 8 * k, column_index), second[k]) for k in range(2)])
            for level in range(2):
                right[level, 0, at : at + 16] = both[0][level]
                right[level, 1, at : at + 16] = -both[1][level]
                right[level, 0, wide + at : wide + at + 16] = both[1][level]
                right[level, 1, wide + at : wide + at + 16] = both[0][level]

    def add(tile, parity, side):
        left, right = left_refs[parity][side], right_refs[parity][side]
        owner = owner_ref[tile]
        product = lax.dot_general(
            jnp.concatenate([left[level, part] for level in (0, 1, 0) for part in range(2)], axis=1),
            jnp.concatenate([right[level, part] for level in (0, 0, 1) for part in range(2)], axis=1),
            last_dims,
            preferred_element_type=jnp.float32,
        )
        sum_ref[owner] = sum_ref[owner] + product

    for side in range(2):
        prepare(side, 0, side)
        prepare(2 + side, 1, side)
    for side in range(2):
        build(0, side)

    def four(step, unused):
        for parity in range(2):
            tile = 4 * step + 2 * parity
            for side in range(2):
                add(tile + side, parity, side)
            for side in range(2):
                build(1 - parity, side)
            for side in range(2):
                prepare(tile + 4 + side, parity, side)
        return unused

    lax.fori_loop(0, (tile_total + 3) // 4, four, 0)

    square_sum = jnp.float32(0.0)
    for device in range(groups * members):
        square_sum = square_sum + extra_ref[device, 0, 2 * layer_dev]
    scale = 1.0 / jnp.sqrt(jnp.full((1, wide), square_sum, jnp.float32))
    chunk = 16

    def screen(step, unused):
        at = pl.multiple_of(step * chunk, chunk)
        depth = depth_ref[pl.ds(at, chunk), :]
        total = jnp.zeros((chunk, wide), jnp.float32)
        for region in range(regions):
            layer_depth = extra_ref[region // layer_dev * members, 0, layer_dev + region % layer_dev]
            halves = (2.0 * layer_depth) * depth
            nearest = jnp.round(halves)
            cosine, sine = half_turn(halves - nearest)
            part = sum_ref[region, pl.ds(at, chunk), :wide] * cosine
            part = part - sum_ref[region, pl.ds(at, chunk), wide:] * sine
            total = total + jnp.where((nearest.astype(jnp.int32) & 1) == 1, -part, part)
        out_ref[pl.ds(at, chunk), :] = (total * scale)[:, :columns]
        return unused

    lax.fori_loop(0, rows // chunk, screen, 0)


def body(
    visibilities,
    weights,
    cell_index,
    kernel_index,
    layer_index,
    tile_counts,
    kernel_table,
    layer_depth,
):
    layer_dev = layer_depth.shape[0]
    groups, members = lax.axis_size("wa"), lax.axis_size("bl")
    tiles, samples = cell_index.shape[1:]
    slots = tiles * samples
    rows, columns = GRID // groups, GRID // members
    wide = max(columns, LANES)
    vmem = pl.BlockSpec(memory_space=pltpu.VMEM)
    smem = pl.BlockSpec(memory_space=pltpu.SMEM)
    devices = groups * members
    packed = pl.pallas_call(
        functools.partial(pack_kernel, layer_dev),
        out_shape=jax.ShapeDtypeStruct((devices, FIELDS, slots + LANES), jnp.float32),
        in_specs=[smem, smem, vmem, vmem, vmem, vmem, vmem],
        out_specs=vmem,
        compiler_params=pltpu.CompilerParams(vmem_limit_bytes=4 << 20),
        name="pack_slots",
    )(
        tile_counts,
        layer_depth,
        visibilities.reshape(2 * tiles, samples),
        weights.reshape(tiles, samples),
        cell_index.reshape(tiles, samples),
        kernel_index.reshape(tiles, samples),
        layer_index.reshape(tiles, samples),
    )
    gathered = lax.all_to_all(packed, ("wa", "bl"), split_axis=0, concat_axis=0, tiled=True)
    period = min(rows, LANES)
    steps_u, steps_v = -(-period // 64) * 8, -(-wide // 64) * 8
    shapes = [(2, rows, LANES), (2, 8, LANES), (2, steps_u, LANES)]
    shapes = shapes + [(2, wide, LANES), (2, 8, LANES), (2, steps_v, LANES), (rows, wide)]
    tables = pl.pallas_call(
        table_kernel,
        out_shape=[jax.ShapeDtypeStruct(shape, jnp.float32) for shape in shapes],
        in_specs=[vmem],
        out_specs=[vmem] * len(shapes),
        compiler_params=pltpu.CompilerParams(vmem_limit_bytes=8 << 20),
        cost_estimate=pl.CostEstimate(flops=4000000, bytes_accessed=1000000, transcendentals=0),
        name="lane_tables",
    )(kernel_table.T)
    region_tiles = members * slots // LANES + 2 * (slots // LANES) + 1
    most_tiles = devices * slots // LANES + groups * layer_dev + 8

    def four_of(shape, kind):
        return [[pltpu.VMEM(shape, kind) for side in range(2)] for parity in range(2)]

    return pl.pallas_call(
        functools.partial(image_kernel, layer_dev, groups, members),
        out_shape=jax.ShapeDtypeStruct((rows, columns), jnp.float32),
        in_specs=[vmem] * (1 + len(shapes)),
        out_specs=vmem,
        scratch_shapes=[
            pltpu.SMEM((devices, 1, LANES), jnp.float32),
            pltpu.VMEM((groups * layer_dev * region_tiles, FIELDS, LANES), jnp.float32),
            four_of((8, LANES), jnp.int32),
            four_of((2, 16 + steps_u + steps_v, LANES), jnp.float32),
            four_of((2, 2, rows, LANES), jnp.bfloat16),
            four_of((2, 2, 2 * wide, LANES), jnp.bfloat16),
            pltpu.VMEM((groups * layer_dev, rows, 2 * wide), jnp.float32),
            pltpu.SMEM((most_tiles,), jnp.int32),
            pltpu.SMEM((most_tiles,), jnp.int32),
            pltpu.SMEM((most_tiles,), jnp.int32),
            pltpu.SemaphoreType.DMA,
        ],
        compiler_params=pltpu.CompilerParams(vmem_limit_bytes=24 << 20),
        name="slots_to_image",
    )(gathered, *tables)


def solution(mesh):
    in_specs = (
        P("wa", "bl", None, None),
        P("wa", "bl", None),
        P("wa", "bl", None),
        P("wa", "bl", None),
        P("wa", "bl", None),
        P("wa", "bl"),
        P(),
        P("wa"),
    )
    return jax.shard_map(body, mesh=mesh, in_specs=in_specs, out_specs=P("wa", "bl"), check_vma=False)
```

```python
import functools
import math

import jax
import jax.numpy as jnp
from jax import lax
from jax.experimental import pallas as pl
from jax.experimental.pallas import tpu as pltpu
from jax.sharding import PartitionSpec as P

GRID = 1024
SUPPORT = 8
OVERSAMPLE = 16
FIELD_OF_VIEW = 0.6

LANES = 128
LOW = LANES // OVERSAMPLE
FIELDS = 4
LONG = 4
SENT = 2

highest = lax.Precision.HIGHEST
last_dims = (((1,), (1,)), ((), ()))

COS_TERMS = (0.2196967899799347, -1.3318802118301392, 4.058412075042725, -4.934792995452881, 0.9999999403953552)
SIN_TERMS = (0.0772201269865036, -0.5980451703071594, 2.5500314235687256, -5.1677069664001465, 3.141592502593994)
GRID_BITS = GRID.bit_length() - 1
LOW_BITS = LOW.bit_length() - 1
POSITION_BITS = OVERSAMPLE.bit_length() - 1


def iota(shape, dim):
    return lax.broadcasted_iota(jnp.int32, shape, dim)


def half_turn(value):
    square = value * value
    cosine = jnp.full_like(square, COS_TERMS[0])
    for term in COS_TERMS[1:]:
        cosine = cosine * square + term
    sine = jnp.full_like(square, SIN_TERMS[0])
    for term in SIN_TERMS[1:]:
        sine = sine * square + term
    return cosine, sine * value


def unit_root(power):
    moved = power + GRID // 4
    step = (moved & (GRID // 2 - 1)) - GRID // 4
    cosine, sine = half_turn(step.astype(jnp.float32) * (2.0 / GRID))
    flip = (moved & (GRID // 2)) != 0
    return jnp.where(flip, -cosine, cosine), jnp.where(flip, -sine, sine)


def split_two(value):
    upper = value.astype(jnp.bfloat16)
    return upper, (value - upper.astype(jnp.float32)).astype(jnp.bfloat16)


def pack_kernel(layer_dev, count_ref, depth_ref, vis_ref, weight_ref, cell_ref, kernel_ref, layer_ref, out_ref):
    tiles, samples = weight_ref.shape
    slots = tiles * samples
    lane = iota((1, samples), 1)
    rows = []
    used_weight = []
    for tile in range(tiles):
        used = lane < count_ref[0, tile]
        used_weight.append(jnp.where(used, weight_ref[tile : tile + 1, :], 0.0))
        for layer in range(layer_dev):
            rows.append(jnp.where(used & (layer_ref[tile : tile + 1, :] == layer), 1.0, 0.0))
    mask = jnp.concatenate(rows, axis=0)
    upper = jnp.where(iota((samples, samples), 0) <= iota((samples, samples), 1), 1.0, 0.0)
    rank = jnp.dot(
        mask.astype(jnp.bfloat16), upper.astype(jnp.bfloat16), preferred_element_type=jnp.float32
    )
    total = jnp.sum(mask, axis=1, keepdims=True)
    base = jnp.zeros((1, 1), jnp.float32)
    layer_count = []
    target = [jnp.full((1, samples), -1.0, jnp.float32) for tile in range(tiles)]
    for layer in range(layer_dev):
        start = base
        for tile in range(tiles):
            row = tile * layer_dev + layer
            place = base + rank[row : row + 1, :] - 1.0
            target[tile] = jnp.where(mask[row : row + 1, :] > 0.0, place, target[tile])
            base = base + total[row : row + 1, :]
        layer_count.append(base - start)
    target = jnp.concatenate(target, axis=1).astype(jnp.int32)
    chosen = jnp.where(iota((slots, slots), 0) == target, 1.0, 0.0).astype(jnp.bfloat16)
    weight_row = jnp.concatenate(used_weight, axis=1)
    real_row = jnp.concatenate([vis_ref[2 * t : 2 * t + 1, :] for t in range(tiles)], axis=1)
    imag_row = jnp.concatenate([vis_ref[2 * t + 1 : 2 * t + 2, :] for t in range(tiles)], axis=1)
    cell_row = jnp.concatenate([cell_ref[t : t + 1, :] for t in range(tiles)], axis=1)
    kernel_row = jnp.concatenate([kernel_ref[t : t + 1, :] for t in range(tiles)], axis=1)
    fields = jnp.concatenate(
        [
            real_row * weight_row,
            imag_row * weight_row,
            cell_row.astype(jnp.float32),
            kernel_row.astype(jnp.float32),
        ],
        axis=0,
    )
    parts = []
    for part in range(3):
        upper_part = fields.astype(jnp.bfloat16)
        parts.append(upper_part.astype(jnp.float32))
        fields = fields - upper_part.astype(jnp.float32)
    moved = lax.dot_general(
        jnp.concatenate(parts, axis=0).astype(jnp.bfloat16),
        chosen,
        last_dims,
        preferred_element_type=jnp.float32,
    )
    moved = moved[:FIELDS] + moved[FIELDS : 2 * FIELDS] + moved[2 * FIELDS :]
    wide = iota((SENT, LANES), 1)
    extra = jnp.zeros((SENT, LANES), jnp.float32)
    square = jnp.sum(weight_row * weight_row, axis=1, keepdims=True)
    extra = jnp.where(wide == 2 * layer_dev, square, extra)
    for layer in range(layer_dev):
        extra = jnp.where(wide == layer, layer_count[layer], extra)
        extra = jnp.where(wide == layer_dev + layer, depth_ref[layer], extra)
    for device in range(out_ref.shape[0]):
        for pair in range(FIELDS // SENT):
            out_ref[device, :, pair * slots : (pair + 1) * slots] = moved[SENT * pair : SENT * (pair + 1)]
        out_ref[device, :, FIELDS // SENT * slots :] = extra


def table_kernel(taps_ref, first_u, base_u, step_u, first_v, base_v, step_v, depth_ref):
    rows, columns = depth_ref.shape
    row_start = lax.axis_index("wa") * rows
    column_start = lax.axis_index("bl") * (GRID // lax.axis_size("bl"))
    low_lane = iota((OVERSAMPLE, LANES), 1) & (LOW - 1)
    position_lane = iota((OVERSAMPLE, LANES), 1) >> LOW_BITS
    picked = jnp.where(position_lane == iota((OVERSAMPLE, LANES), 0), 1.0, 0.0)
    taps = jnp.dot(taps_ref[...], picked, precision=highest, preferred_element_type=jnp.float32)
    band = jnp.zeros((OVERSAMPLE, LANES), jnp.float32)
    for tap in range(SUPPORT):
        band = jnp.where(iota((OVERSAMPLE, LANES), 0) - low_lane == tap, taps[tap : tap + 1, :], band)

    def fill(first, base, step, start):
        count = first.shape[1]
        pixel = start + iota((count, OVERSAMPLE), 0)
        roots = unit_root((iota((count, OVERSAMPLE), 1) - SUPPORT // 2) * pixel)
        for part in range(2):
            first[part] = jnp.dot(roots[part], band, precision=highest, preferred_element_type=jnp.float32)
        roots = unit_root(iota((8, LANES), 1) * LOW * (start + iota((8, LANES), 0)))
        for part in range(2):
            base[part] = roots[part]
        count = step.shape[1]
        roots = unit_root(iota((count, LANES), 1) * LOW * 8 * iota((count, LANES), 0))
        for part in range(2):
            step[part] = roots[part]

    fill(first_u, base_u, step_u, row_start)
    fill(first_v, base_v, step_v, column_start)
    pixel_size = FIELD_OF_VIEW / GRID
    x_coord = (row_start + iota((rows, columns), 0) - GRID // 2).astype(jnp.float32) * pixel_size
    y_coord = (column_start + iota((rows, columns), 1) - GRID // 2).astype(jnp.float32) * pixel_size
    depth_ref[...] = jnp.sqrt(jnp.maximum(1.0 - x_coord * x_coord - y_coord * y_coord, 0.0)) - 1.0


def image_kernel(
    layer_dev,
    groups,
    members,
    slot_ref,
    first_u,
    base_u,
    step_u,
    first_v,
    base_v,
    step_v,
    depth_ref,
    out_ref,
    extra_ref,
    stream_ref,
    index_refs,
    wave_refs,
    left_refs,
    right_refs,
    sum_ref,
    start_ref,
    count_ref,
    copy_sem,
):
    rows, columns = out_ref.shape
    wide = first_v.shape[1]
    slots = (slot_ref.shape[2] - LANES) * SENT // FIELDS
    counts_at = slot_ref.shape[2] - LANES
    source_tiles = slots // LANES
    regions = groups * layer_dev
    region_tiles = stream_ref.shape[0] // regions

    copy = pltpu.make_async_copy(slot_ref.at[:, pl.ds(0, 1), pl.ds(counts_at, LANES)], extra_ref, copy_sem)
    copy.start()
    sum_ref[...] = jnp.zeros_like(sum_ref)

    lane = iota((FIELDS, LANES), 1)

    def join(group, filled_tiles):
        base = [0] * layer_dev
        for member in range(members):
            device = group * members + member
            source = []
            for t in range(source_tiles):
                pieces = [
                    slot_ref[device, :, slots * pair + LANES * t : slots * pair + LANES * (t + 1)]
                    for pair in range(FIELDS // SENT)
                ]
                source.append(jnp.concatenate(pieces, axis=0))
            origin = 0
            for layer in range(layer_dev):
                count = slot_ref[device, 0, counts_at + layer].astype(jnp.int32)
                offset = base[layer] - origin
                shift = offset & (LANES - 1)
                tile = offset >> 7
                turned = [pltpu.roll(part, shift, 1) for part in source]
                region = (group * layer_dev + layer) * region_tiles + source_tiles
                for t in range(source_tiles + 1):
                    if t == 0:
                        value = turned[0]
                    elif t == source_tiles:
                        value = turned[t - 1]
                    else:
                        value = jnp.where(lane >= shift, turned[t], turned[t - 1])
                    where = region + tile + t
                    keep = lane < base[layer] - (tile + t) * LANES
                    stream_ref[where] = jnp.where(keep, stream_ref[where], value)
                base[layer] = base[layer] + count
                origin = origin + count
        for layer in range(layer_dev):
            region = group * layer_dev + layer
            start_ref[region] = filled_tiles
            count_ref[region] = base[layer]
            filled_tiles = filled_tiles + ((base[layer] + LANES - 1) >> 7)
        return filled_tiles

    tile_total = 0
    for group in range(groups):
        tile_total = join(group, tile_total)

    def find(tile):
        region = 0
        for other in range(1, regions):
            region = region + jnp.where(tile >= start_ref[other], 1, 0)
        first = start_ref[region]
        valid = jnp.where(tile < tile_total, count_ref[region] - (tile - first) * LANES, 0)
        place = jnp.where(tile < tile_total, tile - first, 0)
        return region, region * region_tiles + source_tiles + place, valid

    steps_u, steps_v = step_u.shape[1], step_v.shape[1]

    def pick(ref, at, index):
        return [
            jnp.take_along_axis(ref[part, at : at + 8], index, axis=1, mode="promise_in_bounds") for part in range(2)
        ]

    def times(one, two):
        return one[0] * two[0] - one[1] * two[1], one[0] * two[1] + one[1] * two[0]

    def prepare(tile, parity, side):
        unused, place, valid = find(tile)
        content = stream_ref[place]
        live = iota((1, LANES), 1) < valid
        cell = jnp.where(live, content[2:3], 0.0).astype(jnp.int32)
        kernel = jnp.where(live, content[3:4], 0.0).astype(jnp.int32)
        row = cell >> GRID_BITS
        column = cell & (GRID - 1)
        index, wave = index_refs[parity][side], wave_refs[parity][side]
        index[0:1] = ((kernel >> POSITION_BITS) << LOW_BITS) + (row & (LOW - 1))
        index[1:2] = ((kernel & (OVERSAMPLE - 1)) << LOW_BITS) + (column & (LOW - 1))
        row_high = jnp.broadcast_to(row >> LOW_BITS, (8, LANES))
        column_high = jnp.broadcast_to(column >> LOW_BITS, (8, LANES))
        value = [jnp.broadcast_to(jnp.where(live, content[part : part + 1], 0.0), (8, LANES)) for part in range(2)]
        bases = (pick(base_u, 0, row_high), times(pick(base_v, 0, column_high), value))
        at = 0
        for base, step, high in zip(bases, (step_u, step_v), (row_high, column_high)):
            for part in range(2):
                wave[part, at : at + 8] = base[part]
            at = at + 8
            for block in range(0, step.shape[1], 8):
                picked = pick(step, block, high)
                for part in range(2):
                    wave[part, at : at + 8] = picked[part]
                at = at + 8

    def build(parity, side):
        left, right = left_refs[parity][side], right_refs[parity][side]
        wave = wave_refs[parity][side]
        row_index, column_index = [
            jnp.broadcast_to(index_refs[parity][side][k : k + 1], (8, LANES)) for k in range(2)
        ]
        row_base = [wave[part, 0:8] for part in range(2)]
        column_base = [wave[part, 8 + steps_u : 16 + steps_u] for part in range(2)]

        def turn(base, at):
            return times(base, [jnp.broadcast_to(wave[part, at : at + 1], (8, LANES)) for part in range(2)])

        def paired(low, high):
            return [split_two(jnp.concatenate([low[part], high[part]], axis=0)) for part in range(2)]

        period = 8 * steps_u
        for at in range(0, period, 16):
            second = [turn(row_base, 8 + (at + half) // 8) for half in (0, 8)]
            for again in range(at, rows, period):
                both = paired(*[times(pick(first_u, again + 8 * k, row_index), second[k]) for k in range(2)])
                for part in range(2):
                    for level in range(2):
                        left[level, part, again : again + 16] = both[part][level]
        for at in range(0, wide, 16):
            second = [turn(column_base, 16 + steps_u + (at + half) // 8) for half in (0, 8)]
            both = paired(*[times(pick(first_v, at + 8 * k, column_index), second[k]) for k in range(2)])
            for level in range(2):
                right[level, 0, at : at + 16] = both[0][level]
                right[level, 1, at : at + 16] = -both[1][level]
                right[level, 0, wide + at : wide + at + 16] = both[1][level]
                right[level, 1, wide + at : wide + at + 16] = both[0][level]

    def add(tile, parity, side):
        left, right = left_refs[parity][side], right_refs[parity][side]
        owner = find(tile)[0]
        product = lax.dot_general(
            jnp.concatenate([left[level, part] for level in (0, 1, 0) for part in range(2)], axis=1),
            jnp.concatenate([right[level, part] for level in (0, 0, 1) for part in range(2)], axis=1),
            last_dims,
            preferred_element_type=jnp.float32,
        )
        sum_ref[owner] = sum_ref[owner] + product

    for side in range(2):
        prepare(side, 0, side)
        prepare(2 + side, 1, side)
    for side in range(2):
        build(0, side)

    def pairs(first_tile, count):
        for pair in range(count):
            parity, tile = pair % 2, first_tile + 2 * pair
            for side in range(2):
                add(tile + side, parity, side)
            for side in range(2):
                build(1 - parity, side)
            for side in range(2):
                prepare(tile + 4 + side, parity, side)

    long_steps = tile_total // (2 * LONG)

    def long_step(step, unused):
        pairs(2 * LONG * step, LONG)
        return unused

    def short_step(step, unused):
        pairs(2 * LONG * long_steps + 4 * step, 2)
        return unused

    lax.fori_loop(0, long_steps, long_step, 0)
    lax.fori_loop(0, (tile_total - 2 * LONG * long_steps + 3) // 4, short_step, 0)
    copy.wait()

    square_sum = jnp.float32(0.0)
    for device in range(groups * members):
        square_sum = square_sum + extra_ref[device, 0, 2 * layer_dev]
    scale = 1.0 / jnp.sqrt(jnp.full((1, wide), square_sum, jnp.float32))
    chunk = 16

    def screen(step, unused):
        at = pl.multiple_of(step * chunk, chunk)
        depth = depth_ref[pl.ds(at, chunk), :]
        total = jnp.zeros((chunk, wide), jnp.float32)
        for region in range(regions):
            layer_depth = extra_ref[region // layer_dev * members, 0, layer_dev + region % layer_dev]
            halves = (2.0 * layer_depth) * depth
            nearest = jnp.round(halves)
            cosine, sine = half_turn(halves - nearest)
            part = sum_ref[region, pl.ds(at, chunk), :wide] * cosine
            part = part - sum_ref[region, pl.ds(at, chunk), wide:] * sine
            total = total + jnp.where((nearest.astype(jnp.int32) & 1) == 1, -part, part)
        out_ref[pl.ds(at, chunk), :] = (total * scale)[:, :columns]
        return unused

    lax.fori_loop(0, rows // chunk, screen, 0)


def body(
    visibilities,
    weights,
    cell_index,
    kernel_index,
    layer_index,
    tile_counts,
    kernel_table,
    layer_depth,
):
    layer_dev = layer_depth.shape[0]
    groups, members = lax.axis_size("wa"), lax.axis_size("bl")
    tiles, samples = cell_index.shape[1:]
    slots = tiles * samples
    rows, columns = GRID // groups, GRID // members
    wide = max(columns, LANES)
    vmem = pl.BlockSpec(memory_space=pltpu.VMEM)
    smem = pl.BlockSpec(memory_space=pltpu.SMEM)
    devices = groups * members
    packed = pl.pallas_call(
        functools.partial(pack_kernel, layer_dev),
        out_shape=jax.ShapeDtypeStruct((devices, SENT, FIELDS // SENT * slots + LANES), jnp.float32),
        in_specs=[smem, smem, vmem, vmem, vmem, vmem, vmem],
        out_specs=vmem,
        name="pack_slots",
    )(
        tile_counts,
        layer_depth,
        visibilities.reshape(2 * tiles, samples),
        weights.reshape(tiles, samples),
        cell_index.reshape(tiles, samples),
        kernel_index.reshape(tiles, samples),
        layer_index.reshape(tiles, samples),
    )
    gathered = lax.all_to_all(packed, ("wa", "bl"), split_axis=0, concat_axis=0, tiled=True)
    period = min(rows, LANES)
    steps_u, steps_v = -(-period // 64) * 8, -(-wide // 64) * 8
    shapes = [(2, rows, LANES), (2, 8, LANES), (2, steps_u, LANES)]
    shapes = shapes + [(2, wide, LANES), (2, 8, LANES), (2, steps_v, LANES), (rows, wide)]
    tables = pl.pallas_call(
        table_kernel,
        out_shape=[jax.ShapeDtypeStruct(shape, jnp.float32) for shape in shapes],
        in_specs=[vmem],
        out_specs=[vmem] * len(shapes),
        compiler_params=pltpu.CompilerParams(vmem_limit_bytes=8 << 20),
        cost_estimate=pl.CostEstimate(flops=4000000, bytes_accessed=1000000, transcendentals=0),
        name="lane_tables",
    )(kernel_table.T)
    region_tiles = members * slots // LANES + 2 * (slots // LANES) + 1

    def four_of(shape, kind):
        return [[pltpu.VMEM(shape, kind) for side in range(2)] for parity in range(2)]

    return pl.pallas_call(
        functools.partial(image_kernel, layer_dev, groups, members),
        out_shape=jax.ShapeDtypeStruct((rows, columns), jnp.float32),
        in_specs=[vmem] * (1 + len(shapes)),
        out_specs=vmem,
        scratch_shapes=[
            pltpu.SMEM((devices, 1, LANES), jnp.float32),
            pltpu.VMEM((groups * layer_dev * region_tiles, FIELDS, LANES), jnp.float32),
            four_of((8, LANES), jnp.int32),
            four_of((2, 16 + steps_u + steps_v, LANES), jnp.float32),
            four_of((2, 2, rows, LANES), jnp.bfloat16),
            four_of((2, 2, 2 * wide, LANES), jnp.bfloat16),
            pltpu.VMEM((groups * layer_dev, rows, 2 * wide), jnp.float32),
            pltpu.SMEM((groups * layer_dev,), jnp.int32),
            pltpu.SMEM((groups * layer_dev,), jnp.int32),
            pltpu.SemaphoreType.DMA,
        ],
        compiler_params=pltpu.CompilerParams(vmem_limit_bytes=24 << 20),
        name="slots_to_image",
    )(gathered, *tables)


def solution(mesh):
    in_specs = (
        P("wa", "bl", None, None),
        P("wa", "bl", None),
        P("wa", "bl", None),
        P("wa", "bl", None),
        P("wa", "bl", None),
        P("wa", "bl"),
        P(),
        P("wa"),
    )
    return jax.shard_map(body, mesh=mesh, in_specs=in_specs, out_specs=P("wa", "bl"), check_vma=False)
```

```python
import functools
import math

import jax
import jax.numpy as jnp
from jax import lax
from jax.experimental import pallas as pl
from jax.experimental.pallas import tpu as pltpu
from jax.sharding import PartitionSpec as P

GRID = 1024
SUPPORT = 8
OVERSAMPLE = 16
FIELD_OF_VIEW = 0.6

LANES = 128
LOW = LANES // OVERSAMPLE
FIELDS = 4
LONG = 4
SENT = 1

highest = lax.Precision.HIGHEST
last_dims = (((1,), (1,)), ((), ()))

COS_TERMS = (0.2196967899799347, -1.3318802118301392, 4.058412075042725, -4.934792995452881, 0.9999999403953552)
SIN_TERMS = (0.0772201269865036, -0.5980451703071594, 2.5500314235687256, -5.1677069664001465, 3.141592502593994)
GRID_BITS = GRID.bit_length() - 1
LOW_BITS = LOW.bit_length() - 1
POSITION_BITS = OVERSAMPLE.bit_length() - 1


def iota(shape, dim):
    return lax.broadcasted_iota(jnp.int32, shape, dim)


def half_turn(value):
    square = value * value
    cosine = jnp.full_like(square, COS_TERMS[0])
    for term in COS_TERMS[1:]:
        cosine = cosine * square + term
    sine = jnp.full_like(square, SIN_TERMS[0])
    for term in SIN_TERMS[1:]:
        sine = sine * square + term
    return cosine, sine * value


def unit_root(power):
    moved = power + GRID // 4
    step = (moved & (GRID // 2 - 1)) - GRID // 4
    cosine, sine = half_turn(step.astype(jnp.float32) * (2.0 / GRID))
    flip = (moved & (GRID // 2)) != 0
    return jnp.where(flip, -cosine, cosine), jnp.where(flip, -sine, sine)


def screens(layer_depth, depth):
    halves = (2.0 * layer_depth) * depth
    nearest = jnp.round(halves)
    cosine, sine = half_turn(halves - nearest)
    return cosine, sine, (nearest.astype(jnp.int32) & 1) == 1


def split_two(value):
    upper = value.astype(jnp.bfloat16)
    return upper, (value - upper.astype(jnp.float32)).astype(jnp.bfloat16)


def pack_kernel(layer_dev, count_ref, depth_ref, vis_ref, weight_ref, cell_ref, kernel_ref, layer_ref, out_ref):
    tiles, samples = weight_ref.shape
    slots = tiles * samples
    lane = iota((1, samples), 1)
    rows = []
    used_weight = []
    for tile in range(tiles):
        used = lane < count_ref[0, tile]
        used_weight.append(jnp.where(used, weight_ref[tile : tile + 1, :], 0.0))
        for layer in range(layer_dev):
            rows.append(jnp.where(used & (layer_ref[tile : tile + 1, :] == layer), 1.0, 0.0))
    mask = jnp.concatenate(rows, axis=0)
    upper = jnp.where(iota((samples, samples), 0) <= iota((samples, samples), 1), 1.0, 0.0)
    rank = jnp.dot(
        mask.astype(jnp.bfloat16), upper.astype(jnp.bfloat16), preferred_element_type=jnp.float32
    )
    total = jnp.sum(mask, axis=1, keepdims=True)
    base = jnp.zeros((1, 1), jnp.float32)
    layer_count = []
    target = [jnp.full((1, samples), -1.0, jnp.float32) for tile in range(tiles)]
    for layer in range(layer_dev):
        start = base
        for tile in range(tiles):
            row = tile * layer_dev + layer
            place = base + rank[row : row + 1, :] - 1.0
            target[tile] = jnp.where(mask[row : row + 1, :] > 0.0, place, target[tile])
            base = base + total[row : row + 1, :]
        layer_count.append(base - start)
    target = jnp.concatenate(target, axis=1).astype(jnp.int32)
    chosen = jnp.where(iota((slots, slots), 0) == target, 1.0, 0.0).astype(jnp.bfloat16)
    weight_row = jnp.concatenate(used_weight, axis=1)
    real_row = jnp.concatenate([vis_ref[2 * t : 2 * t + 1, :] for t in range(tiles)], axis=1)
    imag_row = jnp.concatenate([vis_ref[2 * t + 1 : 2 * t + 2, :] for t in range(tiles)], axis=1)
    cell_row = jnp.concatenate([cell_ref[t : t + 1, :] for t in range(tiles)], axis=1)
    kernel_row = jnp.concatenate([kernel_ref[t : t + 1, :] for t in range(tiles)], axis=1)
    fields = jnp.concatenate(
        [
            real_row * weight_row,
            imag_row * weight_row,
            cell_row.astype(jnp.float32),
            kernel_row.astype(jnp.float32),
        ],
        axis=0,
    )
    parts = []
    for part in range(3):
        upper_part = fields.astype(jnp.bfloat16)
        parts.append(upper_part.astype(jnp.float32))
        fields = fields - upper_part.astype(jnp.float32)
    moved = lax.dot_general(
        jnp.concatenate(parts, axis=0).astype(jnp.bfloat16),
        chosen,
        last_dims,
        preferred_element_type=jnp.float32,
    )
    moved = moved[:FIELDS] + moved[FIELDS : 2 * FIELDS] + moved[2 * FIELDS :]
    wide = iota((SENT, LANES), 1)
    extra = jnp.zeros((SENT, LANES), jnp.float32)
    square = jnp.sum(weight_row * weight_row, axis=1, keepdims=True)
    extra = jnp.where(wide == 2 * layer_dev, square, extra)
    for layer in range(layer_dev):
        extra = jnp.where(wide == layer, layer_count[layer], extra)
        extra = jnp.where(wide == layer_dev + layer, depth_ref[layer], extra)
    for device in range(out_ref.shape[0]):
        for pair in range(FIELDS // SENT):
            out_ref[device, :, pair * slots : (pair + 1) * slots] = moved[SENT * pair : SENT * (pair + 1)]
        out_ref[device, :, FIELDS // SENT * slots :] = extra


def table_kernel(taps_ref, layer_ref, first_u, base_u, step_u, first_v, base_v, step_v, depth_ref, screen_ref):
    rows, columns = depth_ref.shape
    row_start = lax.axis_index("wa") * rows
    column_start = lax.axis_index("bl") * (GRID // lax.axis_size("bl"))
    low_lane = iota((OVERSAMPLE, LANES), 1) & (LOW - 1)
    position_lane = iota((OVERSAMPLE, LANES), 1) >> LOW_BITS
    picked = jnp.where(position_lane == iota((OVERSAMPLE, LANES), 0), 1.0, 0.0)
    taps = jnp.dot(taps_ref[...], picked, precision=highest, preferred_element_type=jnp.float32)
    band = jnp.zeros((OVERSAMPLE, LANES), jnp.float32)
    for tap in range(SUPPORT):
        band = jnp.where(iota((OVERSAMPLE, LANES), 0) - low_lane == tap, taps[tap : tap + 1, :], band)

    def fill(first, base, step, start):
        count = first.shape[1]
        pixel = start + iota((count, OVERSAMPLE), 0)
        roots = unit_root((iota((count, OVERSAMPLE), 1) - SUPPORT // 2) * pixel)
        for part in range(2):
            first[part] = jnp.dot(roots[part], band, precision=highest, preferred_element_type=jnp.float32)
        roots = unit_root(iota((8, LANES), 1) * LOW * (start + iota((8, LANES), 0)))
        for part in range(2):
            base[part] = roots[part]
        count = step.shape[1]
        roots = unit_root(iota((count, LANES), 1) * LOW * 8 * iota((count, LANES), 0))
        for part in range(2):
            step[part] = roots[part]

    fill(first_u, base_u, step_u, row_start)
    fill(first_v, base_v, step_v, column_start)
    pixel_size = FIELD_OF_VIEW / GRID
    x_coord = (row_start + iota((rows, columns), 0) - GRID // 2).astype(jnp.float32) * pixel_size
    y_coord = (column_start + iota((rows, columns), 1) - GRID // 2).astype(jnp.float32) * pixel_size
    depth = jnp.sqrt(jnp.maximum(1.0 - x_coord * x_coord - y_coord * y_coord, 0.0)) - 1.0
    depth_ref[...] = depth
    for layer in range(screen_ref.shape[0]):
        cosine, sine, odd = screens(layer_ref[layer], depth)
        screen_ref[layer, 0] = jnp.where(odd, -cosine, cosine)
        screen_ref[layer, 1] = jnp.where(odd, -sine, sine)


def image_kernel(
    layer_dev,
    groups,
    members,
    slot_ref,
    first_u,
    base_u,
    step_u,
    first_v,
    base_v,
    step_v,
    depth_ref,
    screen_ref,
    out_ref,
    extra_ref,
    stream_ref,
    index_refs,
    wave_refs,
    left_refs,
    right_refs,
    sum_ref,
    start_ref,
    count_ref,
    copy_sem,
):
    rows, columns = out_ref.shape
    wide = first_v.shape[1]
    slots = (slot_ref.shape[2] - LANES) * SENT // FIELDS
    counts_at = slot_ref.shape[2] - LANES
    source_tiles = slots // LANES
    regions = groups * layer_dev
    region_tiles = stream_ref.shape[0] // regions

    copy = pltpu.make_async_copy(slot_ref.at[:, pl.ds(0, 1), pl.ds(counts_at, LANES)], extra_ref, copy_sem)
    copy.start()
    sum_ref[...] = jnp.zeros_like(sum_ref)

    lane = iota((FIELDS, LANES), 1)

    def join(group, filled_tiles):
        base = [0] * layer_dev
        for member in range(members):
            device = group * members + member
            source = []
            for t in range(source_tiles):
                pieces = [
                    slot_ref[device, :, slots * pair + LANES * t : slots * pair + LANES * (t + 1)]
                    for pair in range(FIELDS // SENT)
                ]
                source.append(jnp.concatenate(pieces, axis=0))
            origin = 0
            for layer in range(layer_dev):
                count = slot_ref[device, 0, counts_at + layer].astype(jnp.int32)
                offset = base[layer] - origin
                shift = offset & (LANES - 1)
                tile = offset >> 7
                turned = [pltpu.roll(part, shift, 1) for part in source]
                region = (group * layer_dev + layer) * region_tiles + source_tiles
                for t in range(source_tiles + 1):
                    if t == 0:
                        value = turned[0]
                    elif t == source_tiles:
                        value = turned[t - 1]
                    else:
                        value = jnp.where(lane >= shift, turned[t], turned[t - 1])
                    where = region + tile + t
                    keep = lane < base[layer] - (tile + t) * LANES
                    stream_ref[where] = jnp.where(keep, stream_ref[where], value)
                base[layer] = base[layer] + count
                origin = origin + count
        for layer in range(layer_dev):
            region = group * layer_dev + layer
            start_ref[region] = filled_tiles
            count_ref[region] = base[layer]
            filled_tiles = filled_tiles + ((base[layer] + LANES - 1) >> 7)
        return filled_tiles

    tile_total = 0
    for group in range(groups):
        tile_total = join(group, tile_total)

    def find(tile):
        region = 0
        for other in range(1, regions):
            region = region + jnp.where(tile >= start_ref[other], 1, 0)
        first = start_ref[region]
        valid = jnp.where(tile < tile_total, count_ref[region] - (tile - first) * LANES, 0)
        place = jnp.where(tile < tile_total, tile - first, 0)
        return region, region * region_tiles + source_tiles + place, valid

    steps_u, steps_v = step_u.shape[1], step_v.shape[1]

    def pick(ref, at, index):
        return [
            jnp.take_along_axis(ref[part, at : at + 8], index, axis=1, mode="promise_in_bounds") for part in range(2)
        ]

    def times(one, two):
        return one[0] * two[0] - one[1] * two[1], one[0] * two[1] + one[1] * two[0]

    def prepare(tile, parity, side):
        unused, place, valid = find(tile)
        content = stream_ref[place]
        live = iota((1, LANES), 1) < valid
        cell = jnp.where(live, content[2:3], 0.0).astype(jnp.int32)
        kernel = jnp.where(live, content[3:4], 0.0).astype(jnp.int32)
        row = cell >> GRID_BITS
        column = cell & (GRID - 1)
        index, wave = index_refs[parity][side], wave_refs[parity][side]
        index[0:1] = ((kernel >> POSITION_BITS) << LOW_BITS) + (row & (LOW - 1))
        index[1:2] = ((kernel & (OVERSAMPLE - 1)) << LOW_BITS) + (column & (LOW - 1))
        row_high = jnp.broadcast_to(row >> LOW_BITS, (8, LANES))
        column_high = jnp.broadcast_to(column >> LOW_BITS, (8, LANES))
        value = [jnp.broadcast_to(jnp.where(live, content[part : part + 1], 0.0), (8, LANES)) for part in range(2)]
        bases = (pick(base_u, 0, row_high), times(pick(base_v, 0, column_high), value))
        at = 0
        for base, step, high in zip(bases, (step_u, step_v), (row_high, column_high)):
            for part in range(2):
                wave[part, at : at + 8] = base[part]
            at = at + 8
            for block in range(0, step.shape[1], 8):
                picked = pick(step, block, high)
                for part in range(2):
                    wave[part, at : at + 8] = picked[part]
                at = at + 8

    def build(parity, side):
        left, right = left_refs[parity][side], right_refs[parity][side]
        wave = wave_refs[parity][side]
        row_index, column_index = [
            jnp.broadcast_to(index_refs[parity][side][k : k + 1], (8, LANES)) for k in range(2)
        ]
        row_base = [wave[part, 0:8] for part in range(2)]
        column_base = [wave[part, 8 + steps_u : 16 + steps_u] for part in range(2)]

        def turn(base, at):
            return times(base, [jnp.broadcast_to(wave[part, at : at + 1], (8, LANES)) for part in range(2)])

        def paired(low, high):
            return [split_two(jnp.concatenate([low[part], high[part]], axis=0)) for part in range(2)]

        period = 8 * steps_u
        for at in range(0, period, 16):
            second = [turn(row_base, 8 + (at + half) // 8) for half in (0, 8)]
            for again in range(at, rows, period):
                both = paired(*[times(pick(first_u, again + 8 * k, row_index), second[k]) for k in range(2)])
                for part in range(2):
                    for level in range(2):
                        left[level, part, again : again + 16] = both[part][level]
        for at in range(0, wide, 16):
            second = [turn(column_base, 16 + steps_u + (at + half) // 8) for half in (0, 8)]
            both = paired(*[times(pick(first_v, at + 8 * k, column_index), second[k]) for k in range(2)])
            for level in range(2):
                right[level, 0, at : at + 16] = both[0][level]
                right[level, 1, at : at + 16] = -both[1][level]
                right[level, 0, wide + at : wide + at + 16] = both[1][level]
                right[level, 1, wide + at : wide + at + 16] = both[0][level]

    def add(tile, parity, side):
        left, right = left_refs[parity][side], right_refs[parity][side]
        owner = find(tile)[0]
        product = lax.dot_general(
            jnp.concatenate([left[level, part] for level in (0, 1, 0) for part in range(2)], axis=1),
            jnp.concatenate([right[level, part] for level in (0, 0, 1) for part in range(2)], axis=1),
            last_dims,
            preferred_element_type=jnp.float32,
        )
        sum_ref[owner] = sum_ref[owner] + product

    for side in range(2):
        prepare(side, 0, side)
        prepare(2 + side, 1, side)
    for side in range(2):
        build(0, side)

    def pairs(first_tile, count):
        for pair in range(count):
            parity, tile = pair % 2, first_tile + 2 * pair
            for side in range(2):
                add(tile + side, parity, side)
            for side in range(2):
                build(1 - parity, side)
            for side in range(2):
                prepare(tile + 4 + side, parity, side)

    long_steps = tile_total // (2 * LONG)

    def long_step(step, unused):
        pairs(2 * LONG * step, LONG)
        return unused

    def short_step(step, unused):
        pairs(2 * LONG * long_steps + 4 * step, 2)
        return unused

    lax.fori_loop(0, long_steps, long_step, 0)
    lax.fori_loop(0, (tile_total - 2 * LONG * long_steps + 3) // 4, short_step, 0)
    copy.wait()

    square_sum = jnp.float32(0.0)
    for device in range(groups * members):
        square_sum = square_sum + extra_ref[device, 0, 2 * layer_dev]
    scale = 1.0 / jnp.sqrt(jnp.full((1, wide), square_sum, jnp.float32))
    chunk = min(64, rows)
    own_group = lax.axis_index("wa")

    def screen(step, unused):
        at = pl.multiple_of(step * chunk, chunk)
        depth = depth_ref[pl.ds(at, chunk), :]
        total = jnp.zeros((chunk, wide), jnp.float32)
        for turn_on in range(groups):
            group = (own_group + turn_on) % groups
            for layer in range(layer_dev):
                region = group * layer_dev + layer
                real = sum_ref[region, pl.ds(at, chunk), :wide]
                imag = sum_ref[region, pl.ds(at, chunk), wide:]
                if turn_on == 0:
                    total = total + real * screen_ref[layer, 0, pl.ds(at, chunk)]
                    total = total - imag * screen_ref[layer, 1, pl.ds(at, chunk)]
                else:
                    cosine, sine, odd = screens(extra_ref[group * members, 0, layer_dev + layer], depth)
                    part = real * cosine - imag * sine
                    total = total + jnp.where(odd, -part, part)
        out_ref[pl.ds(at, chunk), :] = (total * scale)[:, :columns]
        return unused

    lax.fori_loop(0, rows // chunk, screen, 0)


def body(
    visibilities,
    weights,
    cell_index,
    kernel_index,
    layer_index,
    tile_counts,
    kernel_table,
    layer_depth,
):
    layer_dev = layer_depth.shape[0]
    groups, members = lax.axis_size("wa"), lax.axis_size("bl")
    tiles, samples = cell_index.shape[1:]
    slots = tiles * samples
    rows, columns = GRID // groups, GRID // members
    wide = max(columns, LANES)
    vmem = pl.BlockSpec(memory_space=pltpu.VMEM)
    smem = pl.BlockSpec(memory_space=pltpu.SMEM)
    devices = groups * members
    packed = pl.pallas_call(
        functools.partial(pack_kernel, layer_dev),
        out_shape=jax.ShapeDtypeStruct((devices, SENT, FIELDS // SENT * slots + LANES), jnp.float32),
        in_specs=[smem, smem, vmem, vmem, vmem, vmem, vmem],
        out_specs=vmem,
        name="pack_slots",
    )(
        tile_counts,
        layer_depth,
        visibilities.reshape(2 * tiles, samples),
        weights.reshape(tiles, samples),
        cell_index.reshape(tiles, samples),
        kernel_index.reshape(tiles, samples),
        layer_index.reshape(tiles, samples),
    )
    gathered = lax.all_to_all(packed, ("wa", "bl"), split_axis=0, concat_axis=0, tiled=True)
    period = min(rows, LANES)
    steps_u, steps_v = -(-period // 64) * 8, -(-wide // 64) * 8
    shapes = [(2, rows, LANES), (2, 8, LANES), (2, steps_u, LANES)]
    shapes = shapes + [(2, wide, LANES), (2, 8, LANES), (2, steps_v, LANES), (rows, wide)]
    shapes = shapes + [(layer_dev, 2, rows, wide)]
    tables = pl.pallas_call(
        table_kernel,
        out_shape=[jax.ShapeDtypeStruct(shape, jnp.float32) for shape in shapes],
        in_specs=[vmem, smem],
        out_specs=[vmem] * len(shapes),
        compiler_params=pltpu.CompilerParams(vmem_limit_bytes=8 << 20),
        cost_estimate=pl.CostEstimate(flops=4000000, bytes_accessed=1000000, transcendentals=0),
        name="lane_tables",
    )(kernel_table.T, layer_depth)
    region_tiles = members * slots // LANES + 2 * (slots // LANES) + 1

    def four_of(shape, kind):
        return [[pltpu.VMEM(shape, kind) for side in range(2)] for parity in range(2)]

    return pl.pallas_call(
        functools.partial(image_kernel, layer_dev, groups, members),
        out_shape=jax.ShapeDtypeStruct((rows, columns), jnp.float32),
        in_specs=[vmem] * (1 + len(shapes)),
        out_specs=vmem,
        scratch_shapes=[
            pltpu.SMEM((devices, 1, LANES), jnp.float32),
            pltpu.VMEM((groups * layer_dev * region_tiles, FIELDS, LANES), jnp.float32),
            four_of((8, LANES), jnp.int32),
            four_of((2, 16 + steps_u + steps_v, LANES), jnp.float32),
            four_of((2, 2, rows, LANES), jnp.bfloat16),
            four_of((2, 2, 2 * wide, LANES), jnp.bfloat16),
            pltpu.VMEM((groups * layer_dev, rows, 2 * wide), jnp.float32),
            pltpu.SMEM((groups * layer_dev,), jnp.int32),
            pltpu.SMEM((groups * layer_dev,), jnp.int32),
            pltpu.SemaphoreType.DMA,
        ],
        compiler_params=pltpu.CompilerParams(vmem_limit_bytes=24 << 20),
        name="slots_to_image",
    )(gathered, *tables)


def solution(mesh):
    in_specs = (
        P("wa", "bl", None, None),
        P("wa", "bl", None),
        P("wa", "bl", None),
        P("wa", "bl", None),
        P("wa", "bl", None),
        P("wa", "bl"),
        P(),
        P("wa"),
    )
    return jax.shard_map(body, mesh=mesh, in_specs=in_specs, out_specs=P("wa", "bl"), check_vma=False)
```

```python
import functools
import math

import jax
import jax.numpy as jnp
from jax import lax
from jax.experimental import pallas as pl
from jax.experimental.pallas import tpu as pltpu
from jax.sharding import PartitionSpec as P

GRID = 1024
SUPPORT = 8
OVERSAMPLE = 16
FIELD_OF_VIEW = 0.6

LANES = 128
LOW = LANES // OVERSAMPLE
FIELDS = 4
LONG = 4
SENT = 1

highest = lax.Precision.HIGHEST
last_dims = (((1,), (1,)), ((), ()))

COS_TERMS = (0.2196967899799347, -1.3318802118301392, 4.058412075042725, -4.934792995452881, 0.9999999403953552)
SIN_TERMS = (0.0772201269865036, -0.5980451703071594, 2.5500314235687256, -5.1677069664001465, 3.141592502593994)
GRID_BITS = GRID.bit_length() - 1
LOW_BITS = LOW.bit_length() - 1
POSITION_BITS = OVERSAMPLE.bit_length() - 1


def iota(shape, dim):
    return lax.broadcasted_iota(jnp.int32, shape, dim)


def half_turn(value):
    square = value * value
    cosine = jnp.full_like(square, COS_TERMS[0])
    for term in COS_TERMS[1:]:
        cosine = cosine * square + term
    sine = jnp.full_like(square, SIN_TERMS[0])
    for term in SIN_TERMS[1:]:
        sine = sine * square + term
    return cosine, sine * value


def unit_root(power):
    moved = power + GRID // 4
    step = (moved & (GRID // 2 - 1)) - GRID // 4
    cosine, sine = half_turn(step.astype(jnp.float32) * (2.0 / GRID))
    flip = (moved & (GRID // 2)) != 0
    return jnp.where(flip, -cosine, cosine), jnp.where(flip, -sine, sine)


def screens(layer_depth, depth):
    halves = (2.0 * layer_depth) * depth
    nearest = jnp.round(halves)
    cosine, sine = half_turn(halves - nearest)
    return cosine, sine, (nearest.astype(jnp.int32) & 1) == 1


def split_two(value):
    upper = value.astype(jnp.bfloat16)
    return upper, (value - upper.astype(jnp.float32)).astype(jnp.bfloat16)


def pack_kernel(layer_dev, count_ref, depth_ref, vis_ref, weight_ref, cell_ref, kernel_ref, layer_ref, out_ref):
    tiles, samples = weight_ref.shape
    slots = tiles * samples
    lane = iota((1, samples), 1)
    rows = []
    used_weight = []
    for tile in range(tiles):
        used = lane < count_ref[0, tile]
        used_weight.append(jnp.where(used, weight_ref[tile : tile + 1, :], 0.0))
        for layer in range(layer_dev):
            rows.append(jnp.where(used & (layer_ref[tile : tile + 1, :] == layer), 1.0, 0.0))
    mask = jnp.concatenate(rows, axis=0)
    upper = jnp.where(iota((samples, samples), 0) <= iota((samples, samples), 1), 1.0, 0.0)
    rank = jnp.dot(
        mask.astype(jnp.bfloat16), upper.astype(jnp.bfloat16), preferred_element_type=jnp.float32
    )
    total = jnp.sum(mask, axis=1, keepdims=True)
    base = jnp.zeros((1, 1), jnp.float32)
    layer_count = []
    target = [jnp.full((1, samples), -1.0, jnp.float32) for tile in range(tiles)]
    for layer in range(layer_dev):
        start = base
        for tile in range(tiles):
            row = tile * layer_dev + layer
            place = base + rank[row : row + 1, :] - 1.0
            target[tile] = jnp.where(mask[row : row + 1, :] > 0.0, place, target[tile])
            base = base + total[row : row + 1, :]
        layer_count.append(base - start)
    target = jnp.concatenate(target, axis=1).astype(jnp.int32)
    chosen = jnp.where(iota((slots, slots), 0) == target, 1.0, 0.0).astype(jnp.bfloat16)
    weight_row = jnp.concatenate(used_weight, axis=1)
    real_row = jnp.concatenate([vis_ref[2 * t : 2 * t + 1, :] for t in range(tiles)], axis=1)
    imag_row = jnp.concatenate([vis_ref[2 * t + 1 : 2 * t + 2, :] for t in range(tiles)], axis=1)
    cell_row = jnp.concatenate([cell_ref[t : t + 1, :] for t in range(tiles)], axis=1)
    kernel_row = jnp.concatenate([kernel_ref[t : t + 1, :] for t in range(tiles)], axis=1)
    fields = jnp.concatenate(
        [
            real_row * weight_row,
            imag_row * weight_row,
            cell_row.astype(jnp.float32),
            kernel_row.astype(jnp.float32),
        ],
        axis=0,
    )
    parts = []
    for part in range(3):
        upper_part = fields.astype(jnp.bfloat16)
        parts.append(upper_part.astype(jnp.float32))
        fields = fields - upper_part.astype(jnp.float32)
    moved = lax.dot_general(
        jnp.concatenate(parts, axis=0).astype(jnp.bfloat16),
        chosen,
        last_dims,
        preferred_element_type=jnp.float32,
    )
    moved = moved[:FIELDS] + moved[FIELDS : 2 * FIELDS] + moved[2 * FIELDS :]
    wide = iota((SENT, LANES), 1)
    extra = jnp.zeros((SENT, LANES), jnp.float32)
    square = jnp.sum(weight_row * weight_row, axis=1, keepdims=True)
    extra = jnp.where(wide == 2 * layer_dev, square, extra)
    for layer in range(layer_dev):
        extra = jnp.where(wide == layer, layer_count[layer], extra)
        extra = jnp.where(wide == layer_dev + layer, depth_ref[layer], extra)
    for device in range(out_ref.shape[0]):
        for pair in range(FIELDS // SENT):
            out_ref[device, :, pair * slots : (pair + 1) * slots] = moved[SENT * pair : SENT * (pair + 1)]
        out_ref[device, :, FIELDS // SENT * slots :] = extra


def table_kernel(taps_ref, layer_ref, first_u, base_u, step_u, first_v, base_v, step_v, depth_ref, screen_ref):
    rows, columns = depth_ref.shape
    row_start = lax.axis_index("wa") * rows
    column_start = lax.axis_index("bl") * (GRID // lax.axis_size("bl"))
    low_lane = iota((OVERSAMPLE, LANES), 1) & (LOW - 1)
    position_lane = iota((OVERSAMPLE, LANES), 1) >> LOW_BITS
    picked = jnp.where(position_lane == iota((OVERSAMPLE, LANES), 0), 1.0, 0.0)
    taps = jnp.dot(taps_ref[...], picked, precision=highest, preferred_element_type=jnp.float32)
    band = jnp.zeros((OVERSAMPLE, LANES), jnp.float32)
    for tap in range(SUPPORT):
        band = jnp.where(iota((OVERSAMPLE, LANES), 0) - low_lane == tap, taps[tap : tap + 1, :], band)

    def fill(first, base, step, start):
        count = first.shape[1]
        pixel = start + iota((count, OVERSAMPLE), 0)
        roots = unit_root((iota((count, OVERSAMPLE), 1) - SUPPORT // 2) * pixel)
        for part in range(2):
            first[part] = jnp.dot(roots[part], band, precision=highest, preferred_element_type=jnp.float32)
        roots = unit_root(iota((8, LANES), 1) * LOW * (start + iota((8, LANES), 0)))
        for part in range(2):
            base[part] = roots[part]
        count = step.shape[1]
        roots = unit_root(iota((count, LANES), 1) * LOW * 8 * iota((count, LANES), 0))
        for part in range(2):
            step[part] = roots[part]

    fill(first_u, base_u, step_u, row_start)
    fill(first_v, base_v, step_v, column_start)
    pixel_size = FIELD_OF_VIEW / GRID
    x_coord = (row_start + iota((rows, columns), 0) - GRID // 2).astype(jnp.float32) * pixel_size
    y_coord = (column_start + iota((rows, columns), 1) - GRID // 2).astype(jnp.float32) * pixel_size
    depth = jnp.sqrt(jnp.maximum(1.0 - x_coord * x_coord - y_coord * y_coord, 0.0)) - 1.0
    depth_ref[...] = depth
    for layer in range(screen_ref.shape[0]):
        cosine, sine, odd = screens(layer_ref[layer], depth)
        screen_ref[layer, 0] = jnp.where(odd, -cosine, cosine)
        screen_ref[layer, 1] = jnp.where(odd, -sine, sine)


def image_kernel(
    layer_dev,
    groups,
    members,
    slot_ref,
    first_u,
    base_u,
    step_u,
    first_v,
    base_v,
    step_v,
    depth_ref,
    screen_ref,
    out_ref,
    extra_ref,
    stream_ref,
    index_refs,
    wave_refs,
    left_refs,
    right_refs,
    sum_ref,
    start_ref,
    count_ref,
    copy_sem,
):
    rows, columns = out_ref.shape
    wide = first_v.shape[1]
    slots = (slot_ref.shape[2] - LANES) * SENT // FIELDS
    counts_at = slot_ref.shape[2] - LANES
    source_tiles = slots // LANES
    regions = groups * layer_dev
    region_tiles = stream_ref.shape[0] // regions

    copy = pltpu.make_async_copy(slot_ref.at[:, pl.ds(0, 1), pl.ds(counts_at, LANES)], extra_ref, copy_sem)
    copy.start()
    sum_ref[...] = jnp.zeros_like(sum_ref)

    lane = iota((FIELDS, LANES), 1)

    def join(group, filled_tiles):
        base = [0] * layer_dev
        for member in range(members):
            device = group * members + member
            source = []
            for t in range(source_tiles):
                pieces = [
                    slot_ref[device, :, slots * pair + LANES * t : slots * pair + LANES * (t + 1)]
                    for pair in range(FIELDS // SENT)
                ]
                source.append(jnp.concatenate(pieces, axis=0))
            origin = 0
            for layer in range(layer_dev):
                count = slot_ref[device, 0, counts_at + layer].astype(jnp.int32)
                offset = base[layer] - origin
                shift = offset & (LANES - 1)
                tile = offset >> 7
                turned = [pltpu.roll(part, shift, 1) for part in source]
                region = (group * layer_dev + layer) * region_tiles + source_tiles
                for t in range(source_tiles + 1):
                    if t == 0:
                        value = turned[0]
                    elif t == source_tiles:
                        value = turned[t - 1]
                    else:
                        value = jnp.where(lane >= shift, turned[t], turned[t - 1])
                    where = region + tile + t
                    keep = lane < base[layer] - (tile + t) * LANES
                    stream_ref[where] = jnp.where(keep, stream_ref[where], value)
                base[layer] = base[layer] + count
                origin = origin + count
        for layer in range(layer_dev):
            region = group * layer_dev + layer
            start_ref[region] = filled_tiles
            count_ref[region] = base[layer]
            filled_tiles = filled_tiles + ((base[layer] + LANES - 1) >> 7)
        return filled_tiles

    tile_total = 0
    for group in range(groups):
        tile_total = join(group, tile_total)

    def find(tile):
        region = 0
        for other in range(1, regions):
            region = region + jnp.where(tile >= start_ref[other], 1, 0)
        first = start_ref[region]
        valid = jnp.where(tile < tile_total, count_ref[region] - (tile - first) * LANES, 0)
        place = jnp.where(tile < tile_total, tile - first, 0)
        return region, region * region_tiles + source_tiles + place, valid

    steps_u, steps_v = step_u.shape[1], step_v.shape[1]

    def pick(ref, at, index):
        return [
            jnp.take_along_axis(ref[part, at : at + 8], index, axis=1, mode="promise_in_bounds") for part in range(2)
        ]

    def times(one, two):
        return one[0] * two[0] - one[1] * two[1], one[0] * two[1] + one[1] * two[0]

    def prepare(tile, parity, side):
        unused, place, valid = find(tile)
        content = stream_ref[place]
        live = iota((1, LANES), 1) < valid
        cell = jnp.where(live, content[2:3], 0.0).astype(jnp.int32)
        kernel = jnp.where(live, content[3:4], 0.0).astype(jnp.int32)
        row = cell >> GRID_BITS
        column = cell & (GRID - 1)
        index, wave = index_refs[parity][side], wave_refs[parity][side]
        index[0:1] = ((kernel >> POSITION_BITS) << LOW_BITS) + (row & (LOW - 1))
        index[1:2] = ((kernel & (OVERSAMPLE - 1)) << LOW_BITS) + (column & (LOW - 1))
        row_high = jnp.broadcast_to(row >> LOW_BITS, (8, LANES))
        column_high = jnp.broadcast_to(column >> LOW_BITS, (8, LANES))
        value = [jnp.broadcast_to(jnp.where(live, content[part : part + 1], 0.0), (8, LANES)) for part in range(2)]
        bases = (pick(base_u, 0, row_high), times(pick(base_v, 0, column_high), value))
        at = 0
        for base, step, high in zip(bases, (step_u, step_v), (row_high, column_high)):
            for part in range(2):
                wave[part, at : at + 8] = base[part]
            at = at + 8
            for block in range(0, step.shape[1], 8):
                picked = pick(step, block, high)
                for part in range(2):
                    wave[part, at : at + 8] = picked[part]
                at = at + 8

    def build(parity, side):
        left, right = left_refs[parity][side], right_refs[parity][side]
        wave = wave_refs[parity][side]
        row_index, column_index = [
            jnp.broadcast_to(index_refs[parity][side][k : k + 1], (8, LANES)) for k in range(2)
        ]
        row_base = [wave[part, 0:8] for part in range(2)]
        column_base = [wave[part, 8 + steps_u : 16 + steps_u] for part in range(2)]

        def turn(base, at):
            return times(base, [jnp.broadcast_to(wave[part, at : at + 1], (8, LANES)) for part in range(2)])

        def paired(low, high):
            return [split_two(jnp.concatenate([low[part], high[part]], axis=0)) for part in range(2)]

        period = 8 * steps_u
        for at in range(0, period, 16):
            second = [turn(row_base, 8 + (at + half) // 8) for half in (0, 8)]
            for again in range(at, rows, period):
                both = paired(*[times(pick(first_u, again + 8 * k, row_index), second[k]) for k in range(2)])
                for part in range(2):
                    for level in range(2):
                        left[level, part, again : again + 16] = both[part][level]
        for at in range(0, wide, 16):
            second = [turn(column_base, 16 + steps_u + (at + half) // 8) for half in (0, 8)]
            both = paired(*[times(pick(first_v, at + 8 * k, column_index), second[k]) for k in range(2)])
            for level in range(2):
                right[level, 0, at : at + 16] = both[0][level]
                right[level, 1, at : at + 16] = -both[1][level]
                right[level, 0, wide + at : wide + at + 16] = both[1][level]
                right[level, 1, wide + at : wide + at + 16] = both[0][level]

    def add(tile, parity, side):
        left, right = left_refs[parity][side], right_refs[parity][side]
        owner = find(tile)[0]
        product = lax.dot_general(
            jnp.concatenate([left[level, part] for level in (0, 1, 0) for part in range(2)], axis=1),
            jnp.concatenate([right[level, part] for level in (0, 0, 1) for part in range(2)], axis=1),
            last_dims,
            preferred_element_type=jnp.float32,
        )
        sum_ref[owner] = sum_ref[owner] + product

    for side in range(2):
        prepare(side, 0, side)
        prepare(2 + side, 1, side)
    for side in range(2):
        build(0, side)

    def pairs(first_tile, count):
        for pair in range(count):
            parity, tile = pair % 2, first_tile + 2 * pair
            for side in range(2):
                add(tile + side, parity, side)
            for side in range(2):
                build(1 - parity, side)
            for side in range(2):
                prepare(tile + 4 + side, parity, side)

    long_steps = tile_total // (2 * LONG)

    def long_step(step, unused):
        pairs(2 * LONG * step, LONG)
        return unused

    def short_step(step, unused):
        pairs(2 * LONG * long_steps + 4 * step, 2)
        return unused

    lax.fori_loop(0, long_steps, long_step, 0)
    rest = tile_total - 2 * LONG * long_steps
    short_steps = (rest + 1) // 4
    lax.fori_loop(0, short_steps, short_step, 0)

    @pl.when(rest > 4 * short_steps)
    def last_pair():
        for side in range(2):
            add(2 * LONG * long_steps + 4 * short_steps + side, 0, side)

    copy.wait()

    square_sum = jnp.float32(0.0)
    for device in range(groups * members):
        square_sum = square_sum + extra_ref[device, 0, 2 * layer_dev]
    scale = 1.0 / jnp.sqrt(jnp.full((1, wide), square_sum, jnp.float32))
    chunk = min(64, rows)
    own_group = lax.axis_index("wa")

    def screen(step, unused):
        at = pl.multiple_of(step * chunk, chunk)
        depth = depth_ref[pl.ds(at, chunk), :]
        total = jnp.zeros((chunk, wide), jnp.float32)
        for turn_on in range(groups):
            group = (own_group + turn_on) % groups
            for layer in range(layer_dev):
                region = group * layer_dev + layer
                real = sum_ref[region, pl.ds(at, chunk), :wide]
                imag = sum_ref[region, pl.ds(at, chunk), wide:]
                if turn_on == 0:
                    total = total + real * screen_ref[layer, 0, pl.ds(at, chunk)]
                    total = total - imag * screen_ref[layer, 1, pl.ds(at, chunk)]
                else:
                    cosine, sine, odd = screens(extra_ref[group * members, 0, layer_dev + layer], depth)
                    part = real * cosine - imag * sine
                    total = total + jnp.where(odd, -part, part)
        out_ref[pl.ds(at, chunk), :] = (total * scale)[:, :columns]
        return unused

    lax.fori_loop(0, rows // chunk, screen, 0)


def body(
    visibilities,
    weights,
    cell_index,
    kernel_index,
    layer_index,
    tile_counts,
    kernel_table,
    layer_depth,
):
    layer_dev = layer_depth.shape[0]
    groups, members = lax.axis_size("wa"), lax.axis_size("bl")
    tiles, samples = cell_index.shape[1:]
    slots = tiles * samples
    rows, columns = GRID // groups, GRID // members
    wide = max(columns, LANES)
    vmem = pl.BlockSpec(memory_space=pltpu.VMEM)
    smem = pl.BlockSpec(memory_space=pltpu.SMEM)
    devices = groups * members
    packed = pl.pallas_call(
        functools.partial(pack_kernel, layer_dev),
        out_shape=jax.ShapeDtypeStruct((devices, SENT, FIELDS // SENT * slots + LANES), jnp.float32),
        in_specs=[smem, smem, vmem, vmem, vmem, vmem, vmem],
        out_specs=vmem,
        name="pack_slots",
    )(
        tile_counts,
        layer_depth,
        visibilities.reshape(2 * tiles, samples),
        weights.reshape(tiles, samples),
        cell_index.reshape(tiles, samples),
        kernel_index.reshape(tiles, samples),
        layer_index.reshape(tiles, samples),
    )
    gathered = lax.all_to_all(packed, ("wa", "bl"), split_axis=0, concat_axis=0, tiled=True)
    period = min(rows, LANES)
    steps_u, steps_v = -(-period // 64) * 8, -(-wide // 64) * 8
    shapes = [(2, rows, LANES), (2, 8, LANES), (2, steps_u, LANES)]
    shapes = shapes + [(2, wide, LANES), (2, 8, LANES), (2, steps_v, LANES), (rows, wide)]
    shapes = shapes + [(layer_dev, 2, rows, wide)]
    tables = pl.pallas_call(
        table_kernel,
        out_shape=[jax.ShapeDtypeStruct(shape, jnp.float32) for shape in shapes],
        in_specs=[vmem, smem],
        out_specs=[vmem] * len(shapes),
        compiler_params=pltpu.CompilerParams(vmem_limit_bytes=8 << 20),
        cost_estimate=pl.CostEstimate(flops=4000000, bytes_accessed=1000000, transcendentals=0),
        name="lane_tables",
    )(kernel_table.T, layer_depth)
    region_tiles = members * slots // LANES + 2 * (slots // LANES) + 1

    def four_of(shape, kind):
        return [[pltpu.VMEM(shape, kind) for side in range(2)] for parity in range(2)]

    return pl.pallas_call(
        functools.partial(image_kernel, layer_dev, groups, members),
        out_shape=jax.ShapeDtypeStruct((rows, columns), jnp.float32),
        in_specs=[vmem] * (1 + len(shapes)),
        out_specs=vmem,
        scratch_shapes=[
            pltpu.SMEM((devices, 1, LANES), jnp.float32),
            pltpu.VMEM((groups * layer_dev * region_tiles, FIELDS, LANES), jnp.float32),
            four_of((8, LANES), jnp.int32),
            four_of((2, 16 + steps_u + steps_v, LANES), jnp.float32),
            four_of((2, 2, rows, LANES), jnp.bfloat16),
            four_of((2, 2, 2 * wide, LANES), jnp.bfloat16),
            pltpu.VMEM((groups * layer_dev, rows, 2 * wide), jnp.float32),
            pltpu.SMEM((groups * layer_dev,), jnp.int32),
            pltpu.SMEM((groups * layer_dev,), jnp.int32),
            pltpu.SemaphoreType.DMA,
        ],
        compiler_params=pltpu.CompilerParams(vmem_limit_bytes=24 << 20),
        name="slots_to_image",
    )(gathered, *tables)


def solution(mesh):
    in_specs = (
        P("wa", "bl", None, None),
        P("wa", "bl", None),
        P("wa", "bl", None),
        P("wa", "bl", None),
        P("wa", "bl", None),
        P("wa", "bl"),
        P(),
        P("wa"),
    )
    return jax.shard_map(body, mesh=mesh, in_specs=in_specs, out_specs=P("wa", "bl"), check_vma=False)
```

```python
import functools
import math

import jax
import jax.numpy as jnp
from jax import lax
from jax.experimental import pallas as pl
from jax.experimental.pallas import tpu as pltpu
from jax.sharding import PartitionSpec as P

GRID = 1024
SUPPORT = 8
OVERSAMPLE = 16
FIELD_OF_VIEW = 0.6

LANES = 128
LOW = LANES // OVERSAMPLE
FIELDS = 4
LONG = 4
SENT = 1

highest = lax.Precision.HIGHEST
last_dims = (((1,), (1,)), ((), ()))

COS_TERMS = (0.2196967899799347, -1.3318802118301392, 4.058412075042725, -4.934792995452881, 0.9999999403953552)
SIN_TERMS = (0.0772201269865036, -0.5980451703071594, 2.5500314235687256, -5.1677069664001465, 3.141592502593994)
GRID_BITS = GRID.bit_length() - 1
LOW_BITS = LOW.bit_length() - 1
POSITION_BITS = OVERSAMPLE.bit_length() - 1


def iota(shape, dim):
    return lax.broadcasted_iota(jnp.int32, shape, dim)


def half_turn(value):
    square = value * value
    cosine = jnp.full_like(square, COS_TERMS[0])
    for term in COS_TERMS[1:]:
        cosine = cosine * square + term
    sine = jnp.full_like(square, SIN_TERMS[0])
    for term in SIN_TERMS[1:]:
        sine = sine * square + term
    return cosine, sine * value


def unit_root(power):
    moved = power + GRID // 4
    step = (moved & (GRID // 2 - 1)) - GRID // 4
    cosine, sine = half_turn(step.astype(jnp.float32) * (2.0 / GRID))
    flip = (moved & (GRID // 2)) != 0
    return jnp.where(flip, -cosine, cosine), jnp.where(flip, -sine, sine)


def screens(layer_depth, depth):
    halves = (2.0 * layer_depth) * depth
    nearest = jnp.round(halves)
    cosine, sine = half_turn(halves - nearest)
    return cosine, sine, (nearest.astype(jnp.int32) & 1) == 1


def split_two(value):
    upper = value.astype(jnp.bfloat16)
    return upper, (value - upper.astype(jnp.float32)).astype(jnp.bfloat16)


def pack_kernel(layer_dev, count_ref, depth_ref, vis_ref, weight_ref, cell_ref, kernel_ref, layer_ref, out_ref):
    tiles, samples = weight_ref.shape
    slots = tiles * samples
    lane = iota((1, samples), 1)
    rows = []
    used_weight = []
    for tile in range(tiles):
        used = lane < count_ref[0, tile]
        used_weight.append(jnp.where(used, weight_ref[tile : tile + 1, :], 0.0))
        for layer in range(layer_dev):
            rows.append(jnp.where(used & (layer_ref[tile : tile + 1, :] == layer), 1.0, 0.0))
    mask = jnp.concatenate(rows, axis=0)
    upper = jnp.where(iota((samples, samples), 0) <= iota((samples, samples), 1), 1.0, 0.0)
    rank = jnp.dot(
        mask.astype(jnp.bfloat16), upper.astype(jnp.bfloat16), preferred_element_type=jnp.float32
    )
    total = jnp.sum(mask, axis=1, keepdims=True)
    base = jnp.zeros((1, 1), jnp.float32)
    layer_count = []
    target = [jnp.full((1, samples), -1.0, jnp.float32) for tile in range(tiles)]
    for layer in range(layer_dev):
        start = base
        for tile in range(tiles):
            row = tile * layer_dev + layer
            place = base + rank[row : row + 1, :] - 1.0
            target[tile] = jnp.where(mask[row : row + 1, :] > 0.0, place, target[tile])
            base = base + total[row : row + 1, :]
        layer_count.append(base - start)
    target = jnp.concatenate(target, axis=1).astype(jnp.int32)
    chosen = jnp.where(iota((slots, slots), 0) == target, 1.0, 0.0).astype(jnp.bfloat16)
    weight_row = jnp.concatenate(used_weight, axis=1)
    real_row = jnp.concatenate([vis_ref[2 * t : 2 * t + 1, :] for t in range(tiles)], axis=1)
    imag_row = jnp.concatenate([vis_ref[2 * t + 1 : 2 * t + 2, :] for t in range(tiles)], axis=1)
    cell_row = jnp.concatenate([cell_ref[t : t + 1, :] for t in range(tiles)], axis=1)
    kernel_row = jnp.concatenate([kernel_ref[t : t + 1, :] for t in range(tiles)], axis=1)
    fields = jnp.concatenate(
        [
            real_row * weight_row,
            imag_row * weight_row,
            cell_row.astype(jnp.float32),
            kernel_row.astype(jnp.float32),
        ],
        axis=0,
    )
    parts = []
    for part in range(3):
        upper_part = fields.astype(jnp.bfloat16)
        parts.append(upper_part.astype(jnp.float32))
        fields = fields - upper_part.astype(jnp.float32)
    moved = lax.dot_general(
        jnp.concatenate(parts, axis=0).astype(jnp.bfloat16),
        chosen,
        last_dims,
        preferred_element_type=jnp.float32,
    )
    moved = moved[:FIELDS] + moved[FIELDS : 2 * FIELDS] + moved[2 * FIELDS :]
    wide = iota((SENT, LANES), 1)
    extra = jnp.zeros((SENT, LANES), jnp.float32)
    square = jnp.sum(weight_row * weight_row, axis=1, keepdims=True)
    extra = jnp.where(wide == 2 * layer_dev, square, extra)
    for layer in range(layer_dev):
        extra = jnp.where(wide == layer, layer_count[layer], extra)
        extra = jnp.where(wide == layer_dev + layer, depth_ref[layer], extra)
    for device in range(out_ref.shape[0]):
        for pair in range(FIELDS // SENT):
            out_ref[device, :, pair * slots : (pair + 1) * slots] = moved[SENT * pair : SENT * (pair + 1)]
        out_ref[device, :, FIELDS // SENT * slots :] = extra


def table_kernel(taps_ref, layer_ref, first_u, base_u, step_u, first_v, base_v, step_v, depth_ref, screen_ref):
    rows, columns = depth_ref.shape
    row_start = lax.axis_index("wa") * rows
    column_start = lax.axis_index("bl") * (GRID // lax.axis_size("bl"))
    low_lane = iota((OVERSAMPLE, LANES), 1) & (LOW - 1)
    position_lane = iota((OVERSAMPLE, LANES), 1) >> LOW_BITS
    picked = jnp.where(position_lane == iota((OVERSAMPLE, LANES), 0), 1.0, 0.0)
    taps = jnp.dot(taps_ref[...], picked, precision=highest, preferred_element_type=jnp.float32)
    band = jnp.zeros((OVERSAMPLE, LANES), jnp.float32)
    for tap in range(SUPPORT):
        band = jnp.where(iota((OVERSAMPLE, LANES), 0) - low_lane == tap, taps[tap : tap + 1, :], band)

    def fill(first, base, step, start):
        count = first.shape[1]
        pixel = start + iota((count, OVERSAMPLE), 0)
        roots = unit_root((iota((count, OVERSAMPLE), 1) - SUPPORT // 2) * pixel)
        for part in range(2):
            first[part] = jnp.dot(roots[part], band, precision=highest, preferred_element_type=jnp.float32)
        roots = unit_root(iota((8, LANES), 1) * LOW * (start + iota((8, LANES), 0)))
        for part in range(2):
            base[part] = roots[part]
        count = step.shape[1]
        roots = unit_root(iota((count, LANES), 1) * LOW * 8 * iota((count, LANES), 0))
        for part in range(2):
            step[part] = roots[part]

    fill(first_u, base_u, step_u, row_start)
    fill(first_v, base_v, step_v, column_start)
    pixel_size = FIELD_OF_VIEW / GRID
    x_coord = (row_start + iota((rows, columns), 0) - GRID // 2).astype(jnp.float32) * pixel_size
    y_coord = (column_start + iota((rows, columns), 1) - GRID // 2).astype(jnp.float32) * pixel_size
    depth = jnp.sqrt(jnp.maximum(1.0 - x_coord * x_coord - y_coord * y_coord, 0.0)) - 1.0
    depth_ref[...] = depth
    for layer in range(screen_ref.shape[0]):
        cosine, sine, odd = screens(layer_ref[layer], depth)
        screen_ref[layer, 0] = jnp.where(odd, -cosine, cosine)
        screen_ref[layer, 1] = jnp.where(odd, -sine, sine)


def image_kernel(
    layer_dev,
    groups,
    members,
    slot_ref,
    first_u,
    base_u,
    step_u,
    first_v,
    base_v,
    step_v,
    depth_ref,
    screen_ref,
    out_ref,
    extra_ref,
    stream_ref,
    index_refs,
    wave_refs,
    left_refs,
    right_refs,
    sum_ref,
    start_ref,
    count_ref,
    copy_sem,
):
    rows, columns = out_ref.shape
    wide = first_v.shape[1]
    slots = (slot_ref.shape[2] - LANES) * SENT // FIELDS
    counts_at = slot_ref.shape[2] - LANES
    source_tiles = slots // LANES
    regions = groups * layer_dev
    region_tiles = stream_ref.shape[0] // regions

    copy = pltpu.make_async_copy(slot_ref.at[:, pl.ds(0, 1), pl.ds(counts_at, LANES)], extra_ref, copy_sem)
    copy.start()
    sum_ref[...] = jnp.zeros_like(sum_ref)

    lane = iota((FIELDS, LANES), 1)

    def join(group, filled_tiles):
        base = [0] * layer_dev
        for member in range(members):
            device = group * members + member
            source = []
            for t in range(source_tiles):
                pieces = [
                    slot_ref[device, :, slots * pair + LANES * t : slots * pair + LANES * (t + 1)]
                    for pair in range(FIELDS // SENT)
                ]
                source.append(jnp.concatenate(pieces, axis=0))
            origin = 0
            for layer in range(layer_dev):
                count = slot_ref[device, 0, counts_at + layer].astype(jnp.int32)
                offset = base[layer] - origin
                shift = offset & (LANES - 1)
                tile = offset >> 7
                turned = [pltpu.roll(part, shift, 1) for part in source]
                region = (group * layer_dev + layer) * region_tiles + source_tiles
                for t in range(source_tiles + 1):
                    if t == 0:
                        value = turned[0]
                    elif t == source_tiles:
                        value = turned[t - 1]
                    else:
                        value = jnp.where(lane >= shift, turned[t], turned[t - 1])
                    where = region + tile + t
                    keep = lane < base[layer] - (tile + t) * LANES
                    stream_ref[where] = jnp.where(keep, stream_ref[where], value)
                base[layer] = base[layer] + count
                origin = origin + count
        for layer in range(layer_dev):
            region = group * layer_dev + layer
            start_ref[region] = filled_tiles
            count_ref[region] = base[layer]
            filled_tiles = filled_tiles + ((base[layer] + LANES - 1) >> 7)
        return filled_tiles

    tile_total = 0
    for group in range(groups):
        tile_total = join(group, tile_total)

    def find(tile):
        region = 0
        for other in range(1, regions):
            region = region + jnp.where(tile >= start_ref[other], 1, 0)
        first = start_ref[region]
        valid = jnp.where(tile < tile_total, count_ref[region] - (tile - first) * LANES, 0)
        place = jnp.where(tile < tile_total, tile - first, 0)
        return region, region * region_tiles + source_tiles + place, valid

    steps_u, steps_v = step_u.shape[1], step_v.shape[1]

    def pick(ref, at, index):
        return [
            jnp.take_along_axis(ref[part, at : at + 8], index, axis=1, mode="promise_in_bounds") for part in range(2)
        ]

    def times(one, two):
        return one[0] * two[0] - one[1] * two[1], one[0] * two[1] + one[1] * two[0]

    def prepare(tile, parity, side):
        unused, place, valid = find(tile)
        content = stream_ref[place]
        live = iota((1, LANES), 1) < valid
        cell = jnp.where(live, content[2:3], 0.0).astype(jnp.int32)
        kernel = jnp.where(live, content[3:4], 0.0).astype(jnp.int32)
        row = cell >> GRID_BITS
        column = cell & (GRID - 1)
        index, wave = index_refs[parity][side], wave_refs[parity][side]
        index[0:1] = ((kernel >> POSITION_BITS) << LOW_BITS) + (row & (LOW - 1))
        index[1:2] = ((kernel & (OVERSAMPLE - 1)) << LOW_BITS) + (column & (LOW - 1))
        row_high = jnp.broadcast_to(row >> LOW_BITS, (8, LANES))
        column_high = jnp.broadcast_to(column >> LOW_BITS, (8, LANES))
        value = [jnp.broadcast_to(jnp.where(live, content[part : part + 1], 0.0), (8, LANES)) for part in range(2)]
        bases = (pick(base_u, 0, row_high), times(pick(base_v, 0, column_high), value))
        at = 0
        for base, step, high in zip(bases, (step_u, step_v), (row_high, column_high)):
            for part in range(2):
                wave[part, at : at + 8] = base[part]
            at = at + 8
            for block in range(0, step.shape[1], 8):
                picked = pick(step, block, high)
                for part in range(2):
                    wave[part, at : at + 8] = picked[part]
                at = at + 8

    def build(parity, side):
        left, right = left_refs[parity][side], right_refs[parity][side]
        wave = wave_refs[parity][side]
        row_index, column_index = [
            jnp.broadcast_to(index_refs[parity][side][k : k + 1], (8, LANES)) for k in range(2)
        ]
        row_base = [wave[part, 0:8] for part in range(2)]
        column_base = [wave[part, 8 + steps_u : 16 + steps_u] for part in range(2)]

        def turn(base, at):
            return times(base, [jnp.broadcast_to(wave[part, at : at + 1], (8, LANES)) for part in range(2)])

        def paired(low, high):
            return [split_two(jnp.concatenate([low[part], high[part]], axis=0)) for part in range(2)]

        period = 8 * steps_u
        for at in range(0, period, 16):
            second = [turn(row_base, 8 + (at + half) // 8) for half in (0, 8)]
            for again in range(at, rows, period):
                both = paired(*[times(pick(first_u, again + 8 * k, row_index), second[k]) for k in range(2)])
                for part in range(2):
                    for level in range(2):
                        left[level, part, again : again + 16] = both[part][level]
        for at in range(0, wide, 16):
            second = [turn(column_base, 16 + steps_u + (at + half) // 8) for half in (0, 8)]
            both = paired(*[times(pick(first_v, at + 8 * k, column_index), second[k]) for k in range(2)])
            for level in range(2):
                right[level, 0, at : at + 16] = both[0][level]
                right[level, 1, at : at + 16] = -both[1][level]
                right[level, 0, wide + at : wide + at + 16] = both[1][level]
                right[level, 1, wide + at : wide + at + 16] = both[0][level]

    def add(tile, parity, side):
        left, right = left_refs[parity][side], right_refs[parity][side]
        owner = find(tile)[0]
        product = lax.dot_general(
            jnp.concatenate([left[level, part] for level in (0, 1, 0) for part in range(2)], axis=1),
            jnp.concatenate([right[level, part] for level in (0, 0, 1) for part in range(2)], axis=1),
            last_dims,
            preferred_element_type=jnp.float32,
        )
        sum_ref[owner] = sum_ref[owner] + product

    for side in range(2):
        prepare(side, 0, side)
        prepare(2 + side, 1, side)
    for side in range(2):
        build(0, side)

    def pairs(first_tile, count):
        for pair in range(count):
            parity, tile = pair % 2, first_tile + 2 * pair
            for side in range(2):
                add(tile + side, parity, side)
            for side in range(2):
                build(1 - parity, side)
            for side in range(2):
                prepare(tile + 4 + side, parity, side)

    long_steps = tile_total // (2 * LONG)

    def long_step(step, unused):
        pairs(2 * LONG * step, LONG)
        return unused

    def short_step(step, unused):
        pairs(2 * LONG * long_steps + 4 * step, 2)
        return unused

    lax.fori_loop(0, long_steps, long_step, 0)
    rest = tile_total - 2 * LONG * long_steps
    short_steps = (rest + 1) // 4
    lax.fori_loop(0, short_steps, short_step, 0)

    @pl.when(rest > 4 * short_steps)
    def last_pair():
        for side in range(2):
            add(2 * LONG * long_steps + 4 * short_steps + side, 0, side)

    copy.wait()

    square_sum = jnp.float32(0.0)
    for device in range(groups * members):
        square_sum = square_sum + extra_ref[device, 0, 2 * layer_dev]
    scale = 1.0 / jnp.sqrt(jnp.full((1, wide), square_sum, jnp.float32))
    chunk = min(128, rows)
    own_group = lax.axis_index("wa")

    def screen(step, unused):
        at = pl.multiple_of(step * chunk, chunk)
        depth = depth_ref[pl.ds(at, chunk), :]
        total = jnp.zeros((chunk, wide), jnp.float32)
        for turn_on in range(groups):
            group = (own_group + turn_on) % groups
            for layer in range(layer_dev):
                region = group * layer_dev + layer
                real = sum_ref[region, pl.ds(at, chunk), :wide]
                imag = sum_ref[region, pl.ds(at, chunk), wide:]
                if turn_on == 0:
                    total = total + real * screen_ref[layer, 0, pl.ds(at, chunk)]
                    total = total - imag * screen_ref[layer, 1, pl.ds(at, chunk)]
                else:
                    cosine, sine, odd = screens(extra_ref[group * members, 0, layer_dev + layer], depth)
                    part = real * cosine - imag * sine
                    total = total + jnp.where(odd, -part, part)
        out_ref[pl.ds(at, chunk), :] = (total * scale)[:, :columns]
        return unused

    lax.fori_loop(0, rows // chunk, screen, 0)


def body(
    visibilities,
    weights,
    cell_index,
    kernel_index,
    layer_index,
    tile_counts,
    kernel_table,
    layer_depth,
):
    layer_dev = layer_depth.shape[0]
    groups, members = lax.axis_size("wa"), lax.axis_size("bl")
    tiles, samples = cell_index.shape[1:]
    slots = tiles * samples
    rows, columns = GRID // groups, GRID // members
    wide = max(columns, LANES)
    vmem = pl.BlockSpec(memory_space=pltpu.VMEM)
    smem = pl.BlockSpec(memory_space=pltpu.SMEM)
    devices = groups * members
    packed = pl.pallas_call(
        functools.partial(pack_kernel, layer_dev),
        out_shape=jax.ShapeDtypeStruct((devices, SENT, FIELDS // SENT * slots + LANES), jnp.float32),
        in_specs=[smem, smem, vmem, vmem, vmem, vmem, vmem],
        out_specs=vmem,
        name="pack_slots",
    )(
        tile_counts,
        layer_depth,
        visibilities.reshape(2 * tiles, samples),
        weights.reshape(tiles, samples),
        cell_index.reshape(tiles, samples),
        kernel_index.reshape(tiles, samples),
        layer_index.reshape(tiles, samples),
    )
    gathered = lax.all_to_all(packed, ("wa", "bl"), split_axis=0, concat_axis=0, tiled=True)
    period = min(rows, LANES)
    steps_u, steps_v = -(-period // 64) * 8, -(-wide // 64) * 8
    shapes = [(2, rows, LANES), (2, 8, LANES), (2, steps_u, LANES)]
    shapes = shapes + [(2, wide, LANES), (2, 8, LANES), (2, steps_v, LANES), (rows, wide)]
    shapes = shapes + [(layer_dev, 2, rows, wide)]
    tables = pl.pallas_call(
        table_kernel,
        out_shape=[jax.ShapeDtypeStruct(shape, jnp.float32) for shape in shapes],
        in_specs=[vmem, smem],
        out_specs=[vmem] * len(shapes),
        compiler_params=pltpu.CompilerParams(vmem_limit_bytes=8 << 20),
        cost_estimate=pl.CostEstimate(flops=4000000, bytes_accessed=1000000, transcendentals=0),
        name="lane_tables",
    )(kernel_table.T, layer_depth)
    region_tiles = members * slots // LANES + 2 * (slots // LANES) + 1

    def four_of(shape, kind):
        return [[pltpu.VMEM(shape, kind) for side in range(2)] for parity in range(2)]

    return pl.pallas_call(
        functools.partial(image_kernel, layer_dev, groups, members),
        out_shape=jax.ShapeDtypeStruct((rows, columns), jnp.float32),
        in_specs=[vmem] * (1 + len(shapes)),
        out_specs=vmem,
        scratch_shapes=[
            pltpu.SMEM((devices, 1, LANES), jnp.float32),
            pltpu.VMEM((groups * layer_dev * region_tiles, FIELDS, LANES), jnp.float32),
            four_of((8, LANES), jnp.int32),
            four_of((2, 16 + steps_u + steps_v, LANES), jnp.float32),
            four_of((2, 2, rows, LANES), jnp.bfloat16),
            four_of((2, 2, 2 * wide, LANES), jnp.bfloat16),
            pltpu.VMEM((groups * layer_dev, rows, 2 * wide), jnp.float32),
            pltpu.SMEM((groups * layer_dev,), jnp.int32),
            pltpu.SMEM((groups * layer_dev,), jnp.int32),
            pltpu.SemaphoreType.DMA,
        ],
        compiler_params=pltpu.CompilerParams(vmem_limit_bytes=24 << 20),
        name="slots_to_image",
    )(gathered, *tables)


def solution(mesh):
    in_specs = (
        P("wa", "bl", None, None),
        P("wa", "bl", None),
        P("wa", "bl", None),
        P("wa", "bl", None),
        P("wa", "bl", None),
        P("wa", "bl"),
        P(),
        P("wa"),
    )
    return jax.shard_map(body, mesh=mesh, in_specs=in_specs, out_specs=P("wa", "bl"), check_vma=False)
```
